32 devices in a mesh: outer: 4 (over y, x), inner: 8 (over z, core).
Axes of the slice: x: 2, y: 2, z: 4, core: 2. Of those that a mesh axis runs over, the one named last changes fastest.
Arguments:
- acts: bfloat16 [32, 2, 512, 512], P(('outer', 'inner')), may hold values from -6 to 6
- cotangent: bfloat16 [32, 2, 512, 512], P(('outer', 'inner')), may hold values from -6 to 6
- residual: float32 [32, 2048, 128], P(('outer', 'inner')), may hold values from -0.6 to 0.6
- owner_residual: float32 [32, 256, 128], P(('outer', 'inner')), may hold values from -3 to 3
- in_count: int32 [32, 2, 8], P(('outer', 'inner')), may hold values from 1 to 128, as said below
- in_rank: int32 [32, 2, 2048], P(('outer', 'inner')), may hold values from 0 to 255, as said below
- out_count: int32 [32, 2], P(('outer', 'inner')), may hold values from 1 to 128
- out_rank: int32 [32, 2, 256], P(('outer', 'inner')), may hold values from 0 to 255, as said below
Outputs:
- applied: bfloat16 [512, 512], replicated
- new_residual: float32 [32, 2048, 128], P(('outer', 'inner'))
- new_owner_residual: float32 [32, 256, 128], P(('outer', 'inner'))
The draws below stay inside these ranges and needn't reach their ends.
Inputs may be any that keep to these rules, and one draw needn't show every extreme that they name: `in_count`: each step has one owner that receives 128 blocks from every replica. `in_rank`: for each replica, step and owner, the ranks of that owner's 256 blocks are a permutation of 0 to 255. `out_rank`: for each replica and step a permutation of 0 to 255.
All inputs are finite; a program needn't handle non-finite values.
Results may differ from the reference program's by a relative error of at most 0.0065.
Values may be sent and summed in bfloat16 or wider, within the bound.
A program may use at most 64 MiB of HBM per device.

```python
import math
import jax
import jax.numpy as jnp
from jax import lax

TILE_R = 512
TILE_C = 512
BLOCK = 128
STEPS = 2
TOK = 512
REPLICAS = 32
BLOCKS = 2048
REGION = 256
CAP = 128
N_OUTER = 4
N_INNER = 8


def skewed_counts(key, shape):
    first = jax.random.randint(jax.random.fold_in(key, 1), shape, 0, CAP)
    second = jax.random.randint(jax.random.fold_in(key, 2), shape, 0, CAP)
    return jnp.minimum(first, second) + 1


def draw_in_count(key, part):
    counts = skewed_counts(jax.random.fold_in(key, 11), (REPLICAS, STEPS, N_INNER))
    hottest = jax.random.randint(jax.random.fold_in(key, 5), (STEPS,), 0, N_INNER)
    owners = jnp.arange(N_INNER)[None, None, :]
    return jnp.where(owners == hottest[None, :, None], CAP, counts).astype(jnp.int32)


def permutations(key, count):
    keys = jax.random.split(key, count)
    return jax.vmap(lambda single: jax.random.permutation(single, REGION))(keys)


def draw_in_rank(key, part):
    ranks = permutations(jax.random.fold_in(key, 13), REPLICAS * STEPS * N_INNER)
    return ranks.reshape(REPLICAS, STEPS, BLOCKS).astype(jnp.int32)


def draw_out_count(key, part):
    counts = skewed_counts(jax.random.fold_in(key, 17), (REPLICAS, STEPS))
    fullest = jax.random.randint(jax.random.fold_in(key, 19), (STEPS,), 0, REPLICAS)
    rows = jnp.arange(REPLICAS)[:, None]
    return jnp.where(rows == fullest[None, :], CAP, counts).astype(jnp.int32)


def draw_out_rank(key, part):
    ranks = permutations(jax.random.fold_in(key, 23), REPLICAS * STEPS)
    return ranks.reshape(REPLICAS, STEPS, REGION).astype(jnp.int32)


def block_scale(key, shape, cuts, smallest, largest):
    factor_of, own = 1.0, jax.random.fold_in(key, 6)
    for axis_at, blocks in cuts:
        draws = jnp.exp(jax.random.uniform(jax.random.fold_in(own, axis_at), (blocks,), jnp.float32, smallest / len(cuts), largest / len(cuts)))
        factor_of = factor_of * jnp.repeat(draws, shape[axis_at] // blocks).reshape([-1 if axis == axis_at else 1 for axis in range(len(shape))])
    return factor_of


def normal_values(rng, shape, width, bound, cuts=(), kind=jnp.bfloat16):
    drawn = width * jax.random.normal(rng, shape, jnp.float32)
    if cuts:
        drawn = drawn * block_scale(rng, shape, cuts, -0.22, 0.18)
    return jnp.clip(drawn, -bound, bound).astype(kind)


def setup_inputs(seed: int = 0) -> dict:
    key_of = jax.random.split(jax.random.key(seed), 9)
    return {
        "acts": normal_values(key_of[0], (REPLICAS, STEPS, TOK, TILE_R), 1.0, 6.0, ((0, 32),)),
        "cotangent": normal_values(key_of[1], (REPLICAS, STEPS, TOK, TILE_C), 1.0, 6.0, ((0, 32),)),
        "residual": normal_values(key_of[2], (REPLICAS, BLOCKS, BLOCK), 0.1, 0.6, ((0, 32),), jnp.float32),
        "owner_residual": normal_values(key_of[3], (REPLICAS, REGION, BLOCK), 0.5, 3.0, ((0, 32),), jnp.float32),
        "in_count": draw_in_count(jax.random.fold_in(key_of[8], 71), 0),
        "in_rank": draw_in_rank(jax.random.fold_in(key_of[8], 71), 0),
        "out_count": draw_out_count(jax.random.fold_in(key_of[8], 71), 0),
        "out_rank": draw_out_rank(jax.random.fold_in(key_of[8], 71), 0),
    }


step_size = 0.0625

def local_grad(pair):
    left, right = pair
    return jnp.einsum('tr,tc->rc', left.astype(jnp.float32), right.astype(jnp.float32), precision=lax.Precision.HIGHEST)

def reference(acts, cotangent, residual, owner_residual, in_count, in_rank, out_count, out_rank):
    scale = 1.0 / math.sqrt(TOK * N_INNER)
    resid = residual
    oresid = owner_residual.reshape(N_OUTER, BLOCKS, BLOCK)
    total = jnp.zeros((BLOCKS, BLOCK), jnp.float32)
    for step in range(STEPS):
        grads = lax.map(local_grad, (acts[:, step], cotangent[:, step]))
        accum = resid + (grads * scale).reshape(REPLICAS, BLOCKS, BLOCK)
        counts = jnp.repeat(in_count[:, step], REGION, axis=1)
        chosen = (in_rank[:, step] < counts)[..., None]
        sent = jnp.where(chosen, accum, jnp.float32(0.0))
        resid = jnp.where(chosen, jnp.float32(0.0), accum)
        pod_sum = lax.optimization_barrier(jnp.sum(sent.reshape(N_OUTER, N_INNER, BLOCKS, BLOCK), axis=1))
        owner_acc = pod_sum + oresid
        ocounts = jnp.repeat(out_count[:, step].reshape(N_OUTER, N_INNER), REGION, axis=1)
        passed = (out_rank[:, step].reshape(N_OUTER, BLOCKS) < ocounts)[..., None]
        cross = lax.optimization_barrier(jnp.sum(jnp.where(passed, owner_acc, jnp.float32(0.0)), axis=0))
        oresid = jnp.where(passed, jnp.float32(0.0), owner_acc)
        delta = cross.astype(jnp.bfloat16)
        total = total + delta.astype(jnp.float32)
    applied = (-step_size * total).astype(jnp.bfloat16).reshape(TILE_R, TILE_C)
    return (applied, resid, oresid.reshape(REPLICAS, REGION, BLOCK))
```

```python
import functools
import math

import jax
import jax.numpy as jnp
from jax import lax
from jax.experimental import pallas as pl
from jax.experimental.pallas import tpu as pltpu
from jax.sharding import PartitionSpec as P

step_size = 0.0625


def select_blocks(resid, grad, ranks_flat, counts, owners, region, width):
    blocks = resid.shape[0]
    accum = (resid + grad.reshape(blocks, width)).reshape(owners, region, width)
    ranks = ranks_flat.reshape(owners, region)
    chosen = (ranks < counts[:, None])[..., None]
    new_resid = jnp.where(chosen, jnp.float32(0.0), accum).reshape(blocks, width)
    return (accum, ranks, chosen, new_resid)


def pack_slots(accum, ranks, counts, slots, region):
    order = lax.iota(jnp.int32, slots)
    picks = (ranks[:, None, :] == order[None, :, None]) & (
        order[None, :, None] < counts[:, None, None]
    )
    picks_f = picks.astype(jnp.float32)
    places = lax.iota(jnp.int32, region).astype(jnp.float32)
    packed = jnp.einsum("nkr,nrd->nkd", picks_f, accum, precision=lax.Precision.HIGHEST)
    where_at = jnp.einsum("nkr,r->nk", picks_f, places, precision=lax.Precision.HIGHEST)
    return (packed, where_at)


def unpack_slots(arrived, spots, region, width):
    places = lax.iota(jnp.int32, region).astype(jnp.float32)
    placed = (spots.reshape(-1)[:, None] == places[None, :]).astype(jnp.float32)
    return jnp.einsum(
        "mr,md->rd", placed, arrived.reshape(-1, width), precision=lax.Precision.HIGHEST
    )


def owner_section(pod_sum, oresid, ranks_out, count_out):
    owner_acc = pod_sum + oresid
    passed = (ranks_out < count_out)[:, None]
    outgoing = jnp.where(passed, owner_acc, jnp.float32(0.0))
    kept = jnp.where(passed, jnp.float32(0.0), owner_acc)
    return (outgoing, kept)


def per_device(acts, cotangent, residual, owner_residual, in_count, in_rank, out_count, out_rank):
    owners = lax.axis_size("inner")
    steps = acts.shape[1]
    tokens = acts.shape[2]
    rows = acts.shape[3]
    cols = cotangent.shape[3]
    blocks = residual.shape[1]
    width = residual.shape[2]
    region = blocks // owners
    slots = max(1, region // 2)
    scale = 1.0 / math.sqrt(tokens * owners)
    resid = residual[0]
    oresid = owner_residual[0]
    crosses = []
    packs = []
    spots_all = []
    for step in range(steps):
        grad = (
            jnp.einsum(
                "tr,tc->rc", acts[0, step], cotangent[0, step], preferred_element_type=jnp.float32
            )
            * scale
        )
        counts = in_count[0, step]
        accum, ranks, chosen, resid = select_blocks(
            resid, grad, in_rank[0, step], counts, owners, region, width
        )
        packed, where_at = pack_slots(accum, ranks, counts, slots, region)
        packs.append(packed)
        spots_all.append(where_at)
    arrived, spots = (
        lax.all_to_all(
            jnp.concatenate(packs, axis=1), "inner", split_axis=0, concat_axis=0, tiled=True
        ),
        lax.all_to_all(
            jnp.concatenate(spots_all, axis=1), "inner", split_axis=0, concat_axis=0, tiled=True
        ),
    )
    outgoings = []
    for step in range(steps):
        pod_sum = unpack_slots(
            arrived[:, step * slots : (step + 1) * slots],
            spots[:, step * slots : (step + 1) * slots],
            region,
            width,
        )
        outgoing, oresid = owner_section(pod_sum, oresid, out_rank[0, step], out_count[0, step])
        outgoings.append(outgoing)
    summed = lax.psum(jnp.stack(outgoings), "outer")
    for step in range(steps):
        crosses.append(summed[step])
    deltas = []
    for cross in crosses:
        delta = cross.astype(jnp.bfloat16)
        deltas.append(lax.all_gather(delta, "inner", axis=0, tiled=True))
    total = deltas[0].astype(jnp.float32)
    for later in deltas[1:]:
        total = total + later.astype(jnp.float32)
    applied = (-step_size * total).astype(jnp.bfloat16)
    return (applied.reshape(rows, cols), resid[None], oresid[None])


LANES = 128
F32 = jnp.float32
BF16 = jnp.bfloat16


def fused_kernel(
    dims,
    acts_hbm, cot_hbm, res_hbm, ores_hbm, cnt_hbm, rank_hbm, ocnt_hbm, orank_hbm,
    ag, resid_ref, nores_ref,
    ores_ref, cnt_ref, rank_ref, ocnt_ref, orank_ref, small_sem,
    acts_v, cot_v, res_v, rk_ref, rp_ref, mt_ref, msend, mrecv, mall_ref, tab_ref,
    sent, psum, tsend, trecv, usend, urecv, osend, orecv, okeep,
    in_sem, ms_sem, mr_sem, ss_sem, sr_sem, ts_sem, tr_sem, us_sem, ur_sem, os_sem, or_sem,
    zs_sem, zr_sem, fs_sem, fr_sem, ps_sem, pr_sem,
):
    n_in, n_out, steps, scale, region, width = dims
    rows, cols = acts_v.shape[2], cot_v.shape[2]
    cpr = cols // width
    rpr = region // cpr
    halves = region // LANES
    rpc = LANES // rpr
    n_z = n_in // 2
    me = lax.axis_index("inner")
    pod = lax.axis_index("outer")
    core = lax.rem(me, 2)
    z = lax.div(me, 2)
    partner = me + 1 - 2 * core

    def outer(d):
        return lax.rem(pod + d, n_out)

    def flip(m):
        v, bit = z, 1
        while bit <= m:
            if m & bit:
                v = v + bit - 2 * bit * lax.rem(lax.div(z, bit), 2)
            bit *= 2
        return v

    def same_core(zz):
        return 2 * zz + core

    far_first = list(range(n_z - 1, 0, -1))

    def remote(src, dst, ssem, rsem, **device):
        return pltpu.make_async_remote_copy(
            src_ref=src, dst_ref=dst, send_sem=ssem, recv_sem=rsem,
            device_id=device, device_id_type=pl.DeviceIdType.MESH,
        )

    sends = []

    def send(*args, **device):
        copy = remote(*args, **device)
        copy.start()
        sends.append(copy)

    def arrive(ref, ssem, rsem, **device):
        remote(ref, ref, ssem, rsem, **device).wait_recv()

    barrier = pltpu.get_barrier_semaphore()
    for m in far_first:
        pl.semaphore_signal(barrier, inc=1, device_id={"inner": same_core(flip(m))}, device_id_type=pl.DeviceIdType.MESH)
    for d in range(1, n_out):
        pl.semaphore_signal(barrier, inc=1, device_id={"outer": outer(d)}, device_id_type=pl.DeviceIdType.MESH)
    pl.semaphore_signal(barrier, inc=1, device_id={"inner": partner}, device_id_type=pl.DeviceIdType.MESH)

    small = [
        pltpu.make_async_copy(src, dst, small_sem.at[k])
        for k, (src, dst) in enumerate(
            ((rank_hbm, rank_ref), (cnt_hbm, cnt_ref), (orank_hbm, orank_ref), (ocnt_hbm, ocnt_ref), (ores_hbm, ores_ref))
        )
    ]
    for copy in small:
        copy.start()
    loads = []
    for s in range(steps):
        pair = [
            pltpu.make_async_copy(acts_hbm.at[s], acts_v.at[s], in_sem.at[2 * s]),
            pltpu.make_async_copy(cot_hbm.at[s], cot_v.at[s], in_sem.at[2 * s + 1]),
        ]
        for copy in pair:
            copy.start()
        loads.append(pair)
        if s == 0:
            res_load = pltpu.make_async_copy(res_hbm, res_v, in_sem.at[2 * steps])
            res_load.start()

    rk_ref[...] = jnp.zeros(rk_ref.shape, F32)
    mall_ref[...] = jnp.zeros(mall_ref.shape, F32)
    msend[...] = jnp.zeros(msend.shape, F32)
    for copy in small:
        copy.wait()
    for s in range(steps):
        for j in range(n_in):
            row = rank_ref[s : s + 1, j * region : (j + 1) * region]
            rk_ref[s * n_in + j : s * n_in + j + 1, :] = jnp.where(row < cnt_ref[s : s + 1, j : j + 1], 1.0, 0.0)
    later = jnp.zeros((1, region), F32)
    for s in reversed(range(steps)):
        later = jnp.where(orank_ref[s : s + 1, :] < ocnt_ref[0:1, s : s + 1], 1.0, later)
        rk_ref[steps * n_in + s : steps * n_in + s + 1, :] = later
    old = lax.broadcasted_iota(jnp.int32, (region, region), 0)
    new = lax.broadcasted_iota(jnp.int32, (region, region), 1)
    shift = rpr.bit_length() - 1
    perm = jnp.where(old == (new & (rpr - 1)) * cpr + (new >> shift), 1.0, 0.0).astype(BF16)
    rp = jnp.dot(rk_ref[...].astype(BF16), perm, preferred_element_type=F32)
    rp_ref[...] = rp

    def eye(n):
        return jnp.where(
            lax.broadcasted_iota(jnp.int32, (n, LANES), 0) == lax.broadcasted_iota(jnp.int32, (n, LANES), 1), 1.0, 0.0
        ).astype(BF16)

    def turned(values):
        return lax.dot_general(
            values.astype(BF16), eye(values.shape[0]), (((0,), (0,)), ((), ())), preferred_element_type=F32
        ).astype(BF16)

    def spread(table, index, n):
        pick = jnp.where(lax.broadcasted_iota(jnp.int32, (LANES, n), 0) == index, 1.0, 0.0).astype(BF16)
        return jnp.dot(table, pick, preferred_element_type=F32)

    mt_ref[...] = turned(rp)
    for s in range(steps):
        for h in range(halves):
            msend[s * halves + h : s * halves + h + 1, :] = rp_ref[
                steps * n_in + s : steps * n_in + s + 1, h * LANES : (h + 1) * LANES
            ]

    def share(s, zz):
        send(sent.at[s, 2 * zz + 1 - core], psum.at[s, zz], ss_sem.at[s, zz], sr_sem.at[s, zz], inner=partner)

    for s in range(steps):
        for copy in loads[s]:
            copy.wait()
        if s == 0:
            res_load.wait()
        for q in range(rows // LANES):
            g = lax.dot_general(
                acts_v[s, :, q * LANES : (q + 1) * LANES], cot_v[s], (((0,), (0,)), ((), ())),
                preferred_element_type=F32,
            ) * scale
            for half in range(rpc):
                j = q * rpc + half
                chosen = spread(mt_ref[...], s * n_in + j, width) > 0.5
                for c in range(cpr):
                    where_at = pl.ds(region * j + c, rpr, stride=cpr)
                    acc = res_v[where_at, :] + g[half * rpr : (half + 1) * rpr, c * width : (c + 1) * width]
                    take = chosen[c * rpr : (c + 1) * rpr]
                    (resid_ref if s == steps - 1 else res_v)[where_at, :] = jnp.where(take, 0.0, acc)
                    sent[s, j, c * rpr : (c + 1) * rpr] = jnp.where(take, acc, 0.0).astype(BF16)
            if s:
                for zz in range(q * rpc // 2, (q + 1) * rpc // 2):
                    share(s, zz)
        if s == 0:
            pl.semaphore_wait(barrier, n_z - 1 + n_out)
            for m in far_first:
                send(msend, mrecv.at[z], ms_sem.at[m], mr_sem.at[z], inner=same_core(flip(m)))
            mrecv[z] = msend[...]
            for zz in range(n_z):
                share(s, zz)

    for m in far_first:
        zz = flip(m)
        arrive(mrecv.at[zz], ms_sem.at[m], mr_sem.at[zz], inner=same_core(zz))
    for zz in range(n_z):
        for s in range(steps):
            for h in range(halves):
                mall_ref[zz * steps + s : zz * steps + s + 1, h * LANES : (h + 1) * LANES] = mrecv[
                    zz, s * halves + h : s * halves + h + 1, :
                ]
    tab_ref[...] = turned(mall_ref[...])
    for s in range(steps):
        for zz in range(n_z):
            arrive(psum.at[s, zz], ss_sem.at[s, zz], sr_sem.at[s, zz], inner=partner)

    for m in far_first + [0]:
        zz = flip(m)
        t = jnp.zeros((region, width), F32)
        o = jnp.zeros((region, width), F32)
        for s in range(steps):
            part = sent[s, same_core(zz)].astype(F32) + psum[s, zz].astype(F32)
            if s == 0 and m == 0:
                part = part + jnp.concatenate([ores_ref[pl.ds(c, rpr, stride=cpr), :] for c in range(cpr)], axis=0)
            passed = spread(tab_ref[...], zz * steps + s, width) > 0.5
            t = t + jnp.where(passed, part, 0.0)
            o = o + jnp.where(passed, 0.0, part)
        for q in range(n_out):
            tsend[zz, q] = t[q * rpr : (q + 1) * rpr].astype(BF16)
        for d in range(1, n_out):
            send(tsend.at[zz, outer(d)], trecv.at[zz, pod], ts_sem.at[m, d], tr_sem.at[zz, pod], outer=outer(d))
        if m:
            osend[zz] = o.astype(BF16)
        else:
            okeep[...] = o
    for m in far_first:
        zz = flip(m)
        send(osend.at[zz], orecv.at[z], os_sem.at[m], or_sem.at[z], inner=same_core(zz))

    for m in far_first + [0]:
        zz = flip(m)
        total = tsend[zz, pod].astype(F32)
        for d in range(1, n_out):
            q = outer(d)
            arrive(trecv.at[zz, q], ts_sem.at[m, d], tr_sem.at[zz, q], outer=q)
            total = total + trecv[zz, q].astype(F32)
        if m:
            usend[zz] = total.astype(BF16)
            send(usend.at[zz], urecv.at[z], us_sem.at[m], ur_sem.at[z], inner=same_core(zz))
    for m in reversed(far_first):
        zz = flip(m)
        arrive(urecv.at[zz], us_sem.at[m], ur_sem.at[zz], inner=same_core(zz))
        total = total + urecv[zz].astype(F32)
    ag[pod, z, core] = (-step_size * total).astype(BF16)

    def forward(m):
        zz = flip(m)
        piece = ag.at[pod, zz, core]
        for d in range(1, n_out):
            send(piece, piece, fs_sem.at[m, d], fr_sem.at[pod, zz], outer=outer(d))

    def hand_over(q, m, d):
        piece = ag.at[q, flip(m), core]
        send(piece, piece, ps_sem.at[m, d], pr_sem.at[q, flip(m)], inner=partner)

    own = ag.at[pod, z, core]
    for m in far_first:
        send(own, own, zs_sem.at[m], zr_sem.at[z], inner=same_core(flip(m)))
    forward(0)
    hand_over(pod, 0, 0)

    kept = okeep[...]
    for m in far_first:
        zz = flip(m)
        arrive(orecv.at[zz], os_sem.at[m], or_sem.at[zz], inner=same_core(zz))
        kept = kept + orecv[zz].astype(F32)
    for c in range(cpr):
        nores_ref[pl.ds(c, rpr, stride=cpr), :] = kept[c * rpr : (c + 1) * rpr]

    for m in reversed(far_first):
        zz = flip(m)
        piece = ag.at[pod, zz, core]
        arrive(piece, zs_sem.at[m], zr_sem.at[zz], inner=same_core(zz))
        forward(m)
        hand_over(pod, m, 0)
    for m in range(n_z):
        for d in range(1, n_out):
            q = outer(d)
            arrive(ag.at[q, flip(m), core], fs_sem.at[m, d], fr_sem.at[q, flip(m)], outer=q)
            hand_over(q, m, d)
    for m in range(n_z):
        for d in range(n_out):
            q = outer(d)
            arrive(ag.at[q, flip(m), 1 - core], ps_sem.at[m, d], pr_sem.at[q, flip(m)], inner=partner)
    for copy in sends:
        copy.wait_send()


def hand_out(pieces, *arrays):
    n = len(arrays)
    pods, rows, width = pieces.shape

    def kernel(*refs):
        src, dst, sems = refs[: n + 1], refs[n + 1 : 2 * n + 2], refs[2 * n + 2]
        copies = [pltpu.make_async_copy(src[k], dst[k], sems.at[k]) for k in range(1, n + 1)]
        copies += [
            pltpu.make_async_copy(src[0].at[q], dst[0].at[:, q * width : (q + 1) * width], sems.at[n + 1 + q])
            for q in range(pods)
        ]
        for copy in copies:
            copy.start()
        for copy in copies:
            copy.wait()

    return pl.pallas_call(
        kernel,
        out_shape=(jax.ShapeDtypeStruct((rows, pods * width), pieces.dtype),)
        + tuple(jax.ShapeDtypeStruct(a.shape, a.dtype) for a in arrays),
        in_specs=[pl.BlockSpec(memory_space=pltpu.VMEM)] * (n + 1),
        out_specs=tuple([pl.BlockSpec(memory_space=pltpu.HBM)] * (n + 1)),
        scratch_shapes=[pltpu.SemaphoreType.DMA((n + 1 + pods,))],
        compiler_params=pltpu.CompilerParams(vmem_limit_bytes=4 << 20),
    )(pieces, *arrays)


def fits(owners, pods, steps, rows, cols, blocks, width, region):
    if width != LANES or region % LANES or region > 256 or cols % width or owners % 4:
        return False
    cpr = cols // width
    rpr = region // cpr
    n_z = owners // 2
    return (
        cpr == pods and cpr * rpr == region and rpr % 16 == 0 and 2 * rpr == LANES
        and rows % LANES == 0 and n_z & (n_z - 1) == 0
        and rpr * owners == rows and steps * (owners + 1) <= LANES and steps * (region // LANES) <= 8
    )


def per_device_fused(acts, cotangent, residual, owner_residual, in_count, in_rank, out_count, out_rank):
    n_in = lax.axis_size("inner")
    n_out = lax.axis_size("outer")
    steps, tokens, rows = acts.shape[1:]
    cols = cotangent.shape[3]
    blocks, width = residual.shape[1:]
    region = blocks // n_in
    if not fits(n_in, n_out, steps, rows, cols, blocks, width, region):
        return per_device(acts, cotangent, residual, owner_residual, in_count, in_rank, out_count, out_rank)
    scale = 1.0 / math.sqrt(tokens * n_in)
    rpr = region // n_out
    n_z = n_in // 2
    n_rk = -(-steps * (n_in + 1) // 16) * 16
    n_ra = -(-steps * n_z // 16) * 16
    vmem = pl.BlockSpec(memory_space=pltpu.VMEM)
    anywhere = pl.BlockSpec(memory_space=pltpu.HBM)
    dma = pltpu.SemaphoreType.DMA
    pieces, resid, oresid = pl.pallas_call(
        functools.partial(fused_kernel, (n_in, n_out, steps, scale, region, width)),
        out_shape=(
            jax.ShapeDtypeStruct((n_out, n_z, 2, rpr, width), BF16),
            jax.ShapeDtypeStruct((blocks, width), F32),
            jax.ShapeDtypeStruct((region, width), F32),
        ),
        in_specs=[anywhere] * 8,
        out_specs=(vmem, vmem, vmem),
        scratch_shapes=[
            pltpu.VMEM((region, width), F32),
            pltpu.VMEM((steps, n_in), jnp.int32),
            pltpu.VMEM((steps, blocks), jnp.int32),
            pltpu.VMEM((1, steps), jnp.int32),
            pltpu.VMEM((steps, region), jnp.int32),
            dma((5,)),
            pltpu.VMEM((steps, tokens, rows), BF16),
            pltpu.VMEM((steps, tokens, cols), BF16),
            pltpu.VMEM((blocks, width), F32),
            pltpu.VMEM((n_rk, region), F32),
            pltpu.VMEM((n_rk, region), F32),
            pltpu.VMEM((region, LANES), BF16),
            pltpu.VMEM((8, LANES), F32),
            pltpu.VMEM((n_z, 8, LANES), F32),
            pltpu.VMEM((n_ra, region), F32),
            pltpu.VMEM((region, LANES), BF16),
            pltpu.VMEM((steps, n_in, region, width), BF16),
            pltpu.VMEM((steps, n_z, region, width), BF16),
            pltpu.VMEM((n_z, n_out, rpr, width), BF16),
            pltpu.VMEM((n_z, n_out, rpr, width), BF16),
            pltpu.VMEM((n_z, rpr, width), BF16),
            pltpu.VMEM((n_z, rpr, width), BF16),
            pltpu.VMEM((n_z, region, width), BF16),
            pltpu.VMEM((n_z, region, width), BF16),
            pltpu.VMEM((region, width), F32),
            dma((2 * steps + 1,)),
            dma((n_z,)),
            dma((n_z,)),
            dma((steps, n_z)),
            dma((steps, n_z)),
            dma((n_z, n_out)),
            dma((n_z, n_out)),
            dma((n_z,)),
            dma((n_z,)),
            dma((n_z,)),
            dma((n_z,)),
            dma((n_z,)),
            dma((n_z,)),
            dma((n_z, n_out)),
            dma((n_out, n_z)),
            dma((n_z, n_out)),
            dma((n_out, n_z)),
        ],
        compiler_params=pltpu.CompilerParams(collective_id=0, has_side_effects=True, vmem_limit_bytes=48 << 20),
    )(*(
        pltpu.with_memory_space_constraint(a, pltpu.HBM)
        for a in (
            acts[0], cotangent[0], residual[0], owner_residual[0], in_count[0], in_rank[0], out_count, out_rank[0]
        )
    ))
    applied, resid, oresid = hand_out(pieces.reshape(n_out, rows, width), resid, oresid)
    return applied, resid[None], oresid[None]


def solution(mesh):
    return jax.shard_map(
        per_device_fused,
        mesh=mesh,
        in_specs=(
            P(("outer", "inner"), None, None, None),
            P(("outer", "inner"), None, None, None),
            P(("outer", "inner"), None, None),
            P(("outer", "inner"), None, None),
            P(("outer", "inner"), None, None),
            P(("outer", "inner"), None, None),
            P(("outer", "inner"), None),
            P(("outer", "inner"), None, None),
        ),
        out_specs=(P(), P(("outer", "inner"), None, None), P(("outer", "inner"), None, None)),
        check_vma=False,
    )
```

```python
import functools
import math

import jax
import jax.numpy as jnp
from jax import lax
from jax.experimental import pallas as pl
from jax.experimental.pallas import tpu as pltpu
from jax.sharding import PartitionSpec as P

step_size = 0.0625


def select_blocks(resid, grad, ranks_flat, counts, owners, region, width):
    blocks = resid.shape[0]
    accum = (resid + grad.reshape(blocks, width)).reshape(owners, region, width)
    ranks = ranks_flat.reshape(owners, region)
    chosen = (ranks < counts[:, None])[..., None]
    new_resid = jnp.where(chosen, jnp.float32(0.0), accum).reshape(blocks, width)
    return (accum, ranks, chosen, new_resid)


def pack_slots(accum, ranks, counts, slots, region):
    order = lax.iota(jnp.int32, slots)
    picks = (ranks[:, None, :] == order[None, :, None]) & (
        order[None, :, None] < counts[:, None, None]
    )
    picks_f = picks.astype(jnp.float32)
    places = lax.iota(jnp.int32, region).astype(jnp.float32)
    packed = jnp.einsum("nkr,nrd->nkd", picks_f, accum, precision=lax.Precision.HIGHEST)
    where_at = jnp.einsum("nkr,r->nk", picks_f, places, precision=lax.Precision.HIGHEST)
    return (packed, where_at)


def unpack_slots(arrived, spots, region, width):
    places = lax.iota(jnp.int32, region).astype(jnp.float32)
    placed = (spots.reshape(-1)[:, None] == places[None, :]).astype(jnp.float32)
    return jnp.einsum(
        "mr,md->rd", placed, arrived.reshape(-1, width), precision=lax.Precision.HIGHEST
    )


def owner_section(pod_sum, oresid, ranks_out, count_out):
    owner_acc = pod_sum + oresid
    passed = (ranks_out < count_out)[:, None]
    outgoing = jnp.where(passed, owner_acc, jnp.float32(0.0))
    kept = jnp.where(passed, jnp.float32(0.0), owner_acc)
    return (outgoing, kept)


def per_device(acts, cotangent, residual, owner_residual, in_count, in_rank, out_count, out_rank):
    owners = lax.axis_size("inner")
    steps = acts.shape[1]
    tokens = acts.shape[2]
    rows = acts.shape[3]
    cols = cotangent.shape[3]
    blocks = residual.shape[1]
    width = residual.shape[2]
    region = blocks // owners
    slots = max(1, region // 2)
    scale = 1.0 / math.sqrt(tokens * owners)
    resid = residual[0]
    oresid = owner_residual[0]
    crosses = []
    packs = []
    spots_all = []
    for step in range(steps):
        grad = (
            jnp.einsum(
                "tr,tc->rc", acts[0, step], cotangent[0, step], preferred_element_type=jnp.float32
            )
            * scale
        )
        counts = in_count[0, step]
        accum, ranks, chosen, resid = select_blocks(
            resid, grad, in_rank[0, step], counts, owners, region, width
        )
        packed, where_at = pack_slots(accum, ranks, counts, slots, region)
        packs.append(packed)
        spots_all.append(where_at)
    arrived, spots = (
        lax.all_to_all(
            jnp.concatenate(packs, axis=1), "inner", split_axis=0, concat_axis=0, tiled=True
        ),
        lax.all_to_all(
            jnp.concatenate(spots_all, axis=1), "inner", split_axis=0, concat_axis=0, tiled=True
        ),
    )
    outgoings = []
    for step in range(steps):
        pod_sum = unpack_slots(
            arrived[:, step * slots : (step + 1) * slots],
            spots[:, step * slots : (step + 1) * slots],
            region,
            width,
        )
        outgoing, oresid = owner_section(pod_sum, oresid, out_rank[0, step], out_count[0, step])
        outgoings.append(outgoing)
    summed = lax.psum(jnp.stack(outgoings), "outer")
    for step in range(steps):
        crosses.append(summed[step])
    deltas = []
    for cross in crosses:
        delta = cross.astype(jnp.bfloat16)
        deltas.append(lax.all_gather(delta, "inner", axis=0, tiled=True))
    total = deltas[0].astype(jnp.float32)
    for later in deltas[1:]:
        total = total + later.astype(jnp.float32)
    applied = (-step_size * total).astype(jnp.bfloat16)
    return (applied.reshape(rows, cols), resid[None], oresid[None])


LANES = 128
F32 = jnp.float32
BF16 = jnp.bfloat16


def fused_kernel(
    dims,
    acts_hbm, cot_hbm, res_hbm, ores_hbm, cnt_hbm, rank_hbm, ocnt_hbm, orank_hbm,
    ag, resid_ref, nores_ref,
    ores_ref, cnt_ref, rank_ref, ocnt_ref, orank_ref,
    acts_v, cot_v, res_v, rk_ref, rp_ref, mt_ref, msend, mrecv, mall_ref, tab_ref,
    sent, psum, tsend, trecv, usend, urecv, osend, orecv, okeep,
    in_sem, s_sem, g_sem, sr_sem, tr_sem, zr_sem, fr_sem,
):
    n_in, n_out, steps, scale, region, width = dims
    rows, cols = acts_v.shape[2], cot_v.shape[2]
    cpr = cols // width
    rpr = region // cpr
    halves = region // LANES
    chunk = 2 * LANES
    rpc = chunk // rpr
    n_z = n_in // 2
    me = lax.axis_index("inner")
    pod = lax.axis_index("outer")
    core = lax.rem(me, 2)
    z = lax.div(me, 2)
    partner = me + 1 - 2 * core
    MASK, SHARE, TOTAL, OVER_Z, KEPT, GATHER_Z, GATHER_O, HAND = range(8)

    def outer(d):
        return lax.rem(pod + d, n_out)

    def flip(m):
        v, bit = z, 1
        while bit <= m:
            if m & bit:
                v = v + bit - 2 * bit * lax.rem(lax.div(z, bit), 2)
            bit *= 2
        return v

    def same_core(zz):
        return 2 * zz + core

    far_first = list(range(n_z - 1, 0, -1))

    def remote(src, dst, ssem, rsem, **device):
        return pltpu.make_async_remote_copy(
            src_ref=src, dst_ref=dst, send_sem=ssem, recv_sem=rsem,
            device_id=device, device_id_type=pl.DeviceIdType.MESH,
        )

    def send(phase, src, dst, rsem, **device):
        remote(src, dst, s_sem.at[phase], rsem, **device).start()

    def arrived(ref, rsem):
        remote(ref, ref, s_sem.at[0], rsem, inner=partner).wait_recv()

    def left(phase, ref):
        remote(ref, ref, s_sem.at[phase], g_sem.at[0], inner=partner).wait_send()

    barrier = pltpu.get_barrier_semaphore()
    for m in far_first:
        pl.semaphore_signal(barrier, inc=1, device_id={"inner": same_core(flip(m))}, device_id_type=pl.DeviceIdType.MESH)
    for d in range(1, n_out):
        pl.semaphore_signal(barrier, inc=1, device_id={"outer": outer(d)}, device_id_type=pl.DeviceIdType.MESH)
    pl.semaphore_signal(barrier, inc=1, device_id={"inner": partner}, device_id_type=pl.DeviceIdType.MESH)

    small = [
        pltpu.make_async_copy(src, dst, in_sem.at[k])
        for k, (src, dst) in enumerate(
            ((rank_hbm, rank_ref), (cnt_hbm, cnt_ref), (orank_hbm, orank_ref), (ocnt_hbm, ocnt_ref), (ores_hbm, ores_ref))
        )
    ]
    for copy in small:
        copy.start()
    loads = []
    for s in range(steps):
        pltpu.make_async_copy(acts_hbm.at[s], acts_v.at[s], in_sem.at[6 + s]).start()
        pltpu.make_async_copy(cot_hbm.at[s], cot_v.at[s], in_sem.at[6 + s]).start()
        if s == 0:
            res_load = pltpu.make_async_copy(res_hbm, res_v, in_sem.at[5])
            res_load.start()

    def loaded(s):
        both = acts_v.at[0:2]
        pltpu.make_async_copy(both, both, in_sem.at[6 + s]).wait()

    rk_ref[...] = jnp.zeros(rk_ref.shape, F32)
    mall_ref[...] = jnp.zeros(mall_ref.shape, F32)
    msend[...] = jnp.zeros(msend.shape, F32)
    for copy in small:
        copy.wait()
    for s in range(steps):
        for j in range(n_in):
            row = rank_ref[s : s + 1, j * region : (j + 1) * region]
            rk_ref[s * n_in + j : s * n_in + j + 1, :] = jnp.where(row < cnt_ref[s : s + 1, j : j + 1], 1.0, 0.0)
    later = jnp.zeros((1, region), F32)
    for s in reversed(range(steps)):
        later = jnp.where(orank_ref[s : s + 1, :] < ocnt_ref[0:1, s : s + 1], 1.0, later)
        rk_ref[steps * n_in + s : steps * n_in + s + 1, :] = later
    old = lax.broadcasted_iota(jnp.int32, (region, region), 0)
    new = lax.broadcasted_iota(jnp.int32, (region, region), 1)
    shift = rpr.bit_length() - 1
    perm = jnp.where(old == (new & (rpr - 1)) * cpr + (new >> shift), 1.0, 0.0).astype(BF16)
    rp = jnp.dot(rk_ref[...].astype(BF16), perm, preferred_element_type=F32)
    rp_ref[...] = rp

    def eye(n):
        return jnp.where(
            lax.broadcasted_iota(jnp.int32, (n, LANES), 0) == lax.broadcasted_iota(jnp.int32, (n, LANES), 1), 1.0, 0.0
        ).astype(BF16)

    def turned(values):
        return lax.dot_general(
            values.astype(BF16), eye(values.shape[0]), (((0,), (0,)), ((), ())), preferred_element_type=F32
        ).astype(BF16)

    def spread(table, index, n):
        pick = jnp.where(lax.broadcasted_iota(jnp.int32, (LANES, n), 0) == index, 1.0, 0.0).astype(BF16)
        return jnp.dot(table, pick, preferred_element_type=F32)

    for s in range(steps):
        for h in range(halves):
            msend[s * halves + h : s * halves + h + 1, :] = rp_ref[
                steps * n_in + s : steps * n_in + s + 1, h * LANES : (h + 1) * LANES
            ]
    mt_ref[...] = turned(rp)

    def greet():
        pl.semaphore_wait(barrier, n_z - 1 + n_out)
        for m in far_first:
            send(MASK, msend, mrecv.at[z], g_sem.at[MASK], inner=same_core(flip(m)))
        mrecv[z] = msend[...]

    def share(s, zz):
        send(SHARE, sent.at[s, 2 * zz + 1 - core], psum.at[s, zz], sr_sem.at[s], inner=partner)

    met = False
    waiting = []
    for s in range(steps):
        if not met and (0, 0) == (s, -1):
            greet()
            met = True
        loaded(s)
        if s == 0:
            res_load.wait()
        for q in range(rows // chunk):
            g = lax.dot_general(
                acts_v[s, :, q * chunk : (q + 1) * chunk], cot_v[s], (((0,), (0,)), ((), ())),
                preferred_element_type=F32,
            ) * scale
            for half in range(rpc):
                j = q * rpc + half
                chosen = spread(mt_ref[...], s * n_in + j, width) > 0.5
                for c in range(cpr):
                    where_at = pl.ds(region * j + c, rpr, stride=cpr)
                    acc = res_v[where_at, :] + g[half * rpr : (half + 1) * rpr, c * width : (c + 1) * width]
                    take = chosen[c * rpr : (c + 1) * rpr]
                    (resid_ref if s == steps - 1 else res_v)[where_at, :] = jnp.where(take, 0.0, acc)
                    sent[s, j, c * rpr : (c + 1) * rpr] = jnp.where(take, acc, 0.0).astype(BF16)
            waiting += [(s, zz) for zz in range(q * rpc // 2, (q + 1) * rpc // 2)]
            if not met and (0, 0) == (s, q):
                greet()
                met = True
            if met:
                for pair in waiting:
                    share(*pair)
                waiting = []

    for s in range(steps):
        arrived(psum.at[s], sr_sem.at[s])

    def split(m):
        zz = flip(m)
        t = jnp.zeros((region, width), F32)
        o = jnp.zeros((region, width), F32)
        for s in range(steps):
            part = sent[s, same_core(zz)].astype(F32) + psum[s, zz].astype(F32)
            if m:
                passed = spread(tab_ref[...], zz * steps + s, width) > 0.5
            else:
                passed = spread(mt_ref[...], steps * n_in + s, width) > 0.5
                if s == 0:
                    part = part + jnp.concatenate([ores_ref[pl.ds(c, rpr, stride=cpr), :] for c in range(cpr)], axis=0)
            t = t + jnp.where(passed, part, 0.0)
            o = o + jnp.where(passed, 0.0, part)
        for q in range(n_out):
            tsend[zz, q] = t[q * rpr : (q + 1) * rpr].astype(BF16)
        for d in range(1, n_out):
            send(TOTAL, tsend.at[zz, outer(d)], trecv.at[zz, pod], tr_sem.at[zz], outer=outer(d))
        if m:
            osend[zz] = o.astype(BF16)
        else:
            okeep[...] = o

    half = region // 2

    def send_kept(m, k):
        zz = flip(m)
        at = pl.ds(k * half, half)
        send(KEPT, osend.at[zz, at], orecv.at[z, at], g_sem.at[KEPT], inner=same_core(zz))

    split(0)
    arrived(mrecv.at[0 : n_z - 1], g_sem.at[MASK])
    for zz in range(n_z):
        for s in range(steps):
            for h in range(halves):
                mall_ref[zz * steps + s : zz * steps + s + 1, h * LANES : (h + 1) * LANES] = mrecv[
                    zz, s * halves + h : s * halves + h + 1, :
                ]
    tab_ref[...] = turned(mall_ref[...])
    for m in far_first:
        split(m)
    late = [(2, 1)]
    for m in far_first:
        for k in range(2):
            if (m, k) not in late:
                send_kept(m, k)

    for m in far_first + [0]:
        zz = flip(m)
        arrived(trecv.at[zz, 0 : n_out - 1], tr_sem.at[zz])
        total = tsend[zz, pod].astype(F32)
        for d in range(1, n_out):
            total = total + trecv[zz, outer(d)].astype(F32)
        if m:
            usend[zz] = total.astype(BF16)
            send(OVER_Z, usend.at[zz], urecv.at[z], g_sem.at[OVER_Z], inner=same_core(zz))
    for part in late:
        send_kept(*part)
    arrived(urecv.at[0 : n_z - 1], g_sem.at[OVER_Z])
    for m in far_first:
        total = total + urecv[flip(m)].astype(F32)
    own = ag.at[pod, z, core]
    own[...] = (-step_size * total).astype(BF16)

    def forward(m):
        zz = flip(m)
        piece = ag.at[pod, zz, core]
        for d in range(1, n_out):
            send(GATHER_O, piece, piece, fr_sem.at[zz], outer=outer(d))

    def hand_over(q, m):
        piece = ag.at[q, flip(m), core]
        send(HAND, piece, piece, g_sem.at[HAND], inner=partner)

    for m in far_first:
        send(GATHER_Z, own, own, zr_sem.at[z], inner=same_core(flip(m)))
    forward(0)
    hand_over(pod, 0)

    arrived(orecv.at[0 : n_z - 1], g_sem.at[KEPT])
    kept = okeep[...]
    for m in far_first:
        kept = kept + orecv[flip(m)].astype(F32)
    for c in range(cpr):
        nores_ref[pl.ds(c, rpr, stride=cpr), :] = kept[c * rpr : (c + 1) * rpr]

    for m in reversed(far_first):
        arrived(ag.at[pod, flip(m), core], zr_sem.at[flip(m)])
        forward(m)
        hand_over(pod, m)
    for m in range(n_z):
        arrived(ag.at[0 : n_out - 1, flip(m), core], fr_sem.at[flip(m)])
        for d in range(1, n_out):
            hand_over(outer(d), m)
    arrived(ag.at[:, :, 1 - core], g_sem.at[HAND])
    left(MASK, mrecv.at[0 : n_z - 1])
    left(SHARE, psum)
    left(TOTAL, trecv.at[:, 0 : n_out - 1])
    left(OVER_Z, urecv.at[0 : n_z - 1])
    left(KEPT, orecv.at[0 : n_z - 1])
    left(GATHER_Z, urecv.at[0 : n_z - 1])
    left(GATHER_O, trecv.at[:, 0 : n_out - 1])
    left(HAND, trecv)


def hand_out(pieces, *arrays):
    n = len(arrays)
    pods, rows, width = pieces.shape

    def kernel(*refs):
        src, dst, sems = refs[: n + 1], refs[n + 1 : 2 * n + 2], refs[2 * n + 2]
        copies = [pltpu.make_async_copy(src[k], dst[k], sems.at[k]) for k in range(1, n + 1)]
        copies += [
            pltpu.make_async_copy(src[0].at[q], dst[0].at[:, q * width : (q + 1) * width], sems.at[n + 1 + q])
            for q in range(pods)
        ]
        for copy in copies:
            copy.start()
        for copy in copies:
            copy.wait()

    return pl.pallas_call(
        kernel,
        out_shape=(jax.ShapeDtypeStruct((rows, pods * width), pieces.dtype),)
        + tuple(jax.ShapeDtypeStruct(a.shape, a.dtype) for a in arrays),
        in_specs=[pl.BlockSpec(memory_space=pltpu.VMEM)] * (n + 1),
        out_specs=tuple([pl.BlockSpec(memory_space=pltpu.HBM)] * (n + 1)),
        scratch_shapes=[pltpu.SemaphoreType.DMA((n + 1 + pods,))],
        compiler_params=pltpu.CompilerParams(vmem_limit_bytes=4 << 20),
    )(pieces, *arrays)


def fits(owners, pods, steps, rows, cols, blocks, width, region):
    if width != LANES or region % LANES or region > 256 or cols % width or owners % 4:
        return False
    cpr = cols // width
    rpr = region // cpr
    n_z = owners // 2
    return (
        cpr == pods and cpr * rpr == region and rpr % 16 == 0 and 2 * rpr == LANES
        and rows % LANES == 0 and n_z & (n_z - 1) == 0
        and rpr * owners == rows and steps * (owners + 1) <= LANES and steps * (region // LANES) <= 8
    )


def per_device_fused(acts, cotangent, residual, owner_residual, in_count, in_rank, out_count, out_rank):
    n_in = lax.axis_size("inner")
    n_out = lax.axis_size("outer")
    steps, tokens, rows = acts.shape[1:]
    cols = cotangent.shape[3]
    blocks, width = residual.shape[1:]
    region = blocks // n_in
    if not fits(n_in, n_out, steps, rows, cols, blocks, width, region):
        return per_device(acts, cotangent, residual, owner_residual, in_count, in_rank, out_count, out_rank)
    scale = 1.0 / math.sqrt(tokens * n_in)
    rpr = region // n_out
    n_z = n_in // 2
    n_rk = -(-steps * (n_in + 1) // 16) * 16
    n_ra = -(-steps * n_z // 16) * 16
    vmem = pl.BlockSpec(memory_space=pltpu.VMEM)
    anywhere = pl.BlockSpec(memory_space=pltpu.HBM)
    dma = pltpu.SemaphoreType.DMA
    pieces, resid, oresid = pl.pallas_call(
        functools.partial(fused_kernel, (n_in, n_out, steps, scale, region, width)),
        out_shape=(
            jax.ShapeDtypeStruct((n_out, n_z, 2, rpr, width), BF16),
            jax.ShapeDtypeStruct((blocks, width), F32),
            jax.ShapeDtypeStruct((region, width), F32),
        ),
        in_specs=[anywhere] * 8,
        out_specs=(vmem, vmem, vmem),
        scratch_shapes=[
            pltpu.VMEM((region, width), F32),
            pltpu.VMEM((steps, n_in), jnp.int32),
            pltpu.VMEM((steps, blocks), jnp.int32),
            pltpu.VMEM((1, steps), jnp.int32),
            pltpu.VMEM((steps, region), jnp.int32),
            pltpu.VMEM((steps, tokens, rows), BF16),
            pltpu.VMEM((steps, tokens, cols), BF16),
            pltpu.VMEM((blocks, width), F32),
            pltpu.VMEM((n_rk, region), F32),
            pltpu.VMEM((n_rk, region), F32),
            pltpu.VMEM((region, LANES), BF16),
            pltpu.VMEM((8, LANES), F32),
            pltpu.VMEM((n_z, 8, LANES), F32),
            pltpu.VMEM((n_ra, region), F32),
            pltpu.VMEM((region, LANES), BF16),
            pltpu.VMEM((steps, n_in, region, width), BF16),
            pltpu.VMEM((steps, n_z, region, width), BF16),
            pltpu.VMEM((n_z, n_out, rpr, width), BF16),
            pltpu.VMEM((n_z, n_out, rpr, width), BF16),
            pltpu.VMEM((n_z, rpr, width), BF16),
            pltpu.VMEM((n_z, rpr, width), BF16),
            pltpu.VMEM((n_z, region, width), BF16),
            pltpu.VMEM((n_z, region, width), BF16),
            pltpu.VMEM((region, width), F32),
            dma((6 + steps,)),
            dma((8,)),
            dma((8,)),
            dma((steps,)),
            dma((n_z,)),
            dma((n_z,)),
            dma((n_z,)),
        ],
        compiler_params=pltpu.CompilerParams(collective_id=0, has_side_effects=True, vmem_limit_bytes=48 << 20),
    )(*(
        pltpu.with_memory_space_constraint(a, pltpu.HBM)
        for a in (
            acts[0], cotangent[0], residual[0], owner_residual[0], in_count[0], in_rank[0], out_count, out_rank[0]
        )
    ))
    applied, resid, oresid = hand_out(pieces.reshape(n_out, rows, width), resid, oresid)
    return applied, resid[None], oresid[None]


def solution(mesh):
    return jax.shard_map(
        per_device_fused,
        mesh=mesh,
        in_specs=(
            P(("outer", "inner"), None, None, None),
            P(("outer", "inner"), None, None, None),
            P(("outer", "inner"), None, None),
            P(("outer", "inner"), None, None),
            P(("outer", "inner"), None, None),
            P(("outer", "inner"), None, None),
            P(("outer", "inner"), None),
            P(("outer", "inner"), None, None),
        ),
        out_specs=(P(), P(("outer", "inner"), None, None), P(("outer", "inner"), None, None)),
        check_vma=False,
    )
```

```python
import functools
import math

import jax
import jax.numpy as jnp
from jax import lax
from jax.experimental import pallas as pl
from jax.experimental.pallas import tpu as pltpu
from jax.sharding import PartitionSpec as P

step_size = 0.0625


def select_blocks(resid, grad, ranks_flat, counts, owners, region, width):
    blocks = resid.shape[0]
    accum = (resid + grad.reshape(blocks, width)).reshape(owners, region, width)
    ranks = ranks_flat.reshape(owners, region)
    chosen = (ranks < counts[:, None])[..., None]
    new_resid = jnp.where(chosen, jnp.float32(0.0), accum).reshape(blocks, width)
    return (accum, ranks, chosen, new_resid)


def pack_slots(accum, ranks, counts, slots, region):
    order = lax.iota(jnp.int32, slots)
    picks = (ranks[:, None, :] == order[None, :, None]) & (
        order[None, :, None] < counts[:, None, None]
    )
    picks_f = picks.astype(jnp.float32)
    places = lax.iota(jnp.int32, region).astype(jnp.float32)
    packed = jnp.einsum("nkr,nrd->nkd", picks_f, accum, precision=lax.Precision.HIGHEST)
    where_at = jnp.einsum("nkr,r->nk", picks_f, places, precision=lax.Precision.HIGHEST)
    return (packed, where_at)


def unpack_slots(arrived, spots, region, width):
    places = lax.iota(jnp.int32, region).astype(jnp.float32)
    placed = (spots.reshape(-1)[:, None] == places[None, :]).astype(jnp.float32)
    return jnp.einsum(
        "mr,md->rd", placed, arrived.reshape(-1, width), precision=lax.Precision.HIGHEST
    )


def owner_section(pod_sum, oresid, ranks_out, count_out):
    owner_acc = pod_sum + oresid
    passed = (ranks_out < count_out)[:, None]
    outgoing = jnp.where(passed, owner_acc, jnp.float32(0.0))
    kept = jnp.where(passed, jnp.float32(0.0), owner_acc)
    return (outgoing, kept)


def per_device(acts, cotangent, residual, owner_residual, in_count, in_rank, out_count, out_rank):
    owners = lax.axis_size("inner")
    steps = acts.shape[1]
    tokens = acts.shape[2]
    rows = acts.shape[3]
    cols = cotangent.shape[3]
    blocks = residual.shape[1]
    width = residual.shape[2]
    region = blocks // owners
    slots = max(1, region // 2)
    scale = 1.0 / math.sqrt(tokens * owners)
    resid = residual[0]
    oresid = owner_residual[0]
    crosses = []
    packs = []
    spots_all = []
    for step in range(steps):
        grad = (
            jnp.einsum(
                "tr,tc->rc", acts[0, step], cotangent[0, step], preferred_element_type=jnp.float32
            )
            * scale
        )
        counts = in_count[0, step]
        accum, ranks, chosen, resid = select_blocks(
            resid, grad, in_rank[0, step], counts, owners, region, width
        )
        packed, where_at = pack_slots(accum, ranks, counts, slots, region)
        packs.append(packed)
        spots_all.append(where_at)
    arrived, spots = (
        lax.all_to_all(
            jnp.concatenate(packs, axis=1), "inner", split_axis=0, concat_axis=0, tiled=True
        ),
        lax.all_to_all(
            jnp.concatenate(spots_all, axis=1), "inner", split_axis=0, concat_axis=0, tiled=True
        ),
    )
    outgoings = []
    for step in range(steps):
        pod_sum = unpack_slots(
            arrived[:, step * slots : (step + 1) * slots],
            spots[:, step * slots : (step + 1) * slots],
            region,
            width,
        )
        outgoing, oresid = owner_section(pod_sum, oresid, out_rank[0, step], out_count[0, step])
        outgoings.append(outgoing)
    summed = lax.psum(jnp.stack(outgoings), "outer")
    for step in range(steps):
        crosses.append(summed[step])
    deltas = []
    for cross in crosses:
        delta = cross.astype(jnp.bfloat16)
        deltas.append(lax.all_gather(delta, "inner", axis=0, tiled=True))
    total = deltas[0].astype(jnp.float32)
    for later in deltas[1:]:
        total = total + later.astype(jnp.float32)
    applied = (-step_size * total).astype(jnp.bfloat16)
    return (applied.reshape(rows, cols), resid[None], oresid[None])


LANES = 128
F32 = jnp.float32
BF16 = jnp.bfloat16


def fused_kernel(
    dims,
    acts_hbm, cot_hbm, res_hbm, ores_hbm, cnt_hbm, rank_hbm, ocnt_hbm, orank_hbm,
    ag, resid_ref, nores_ref,
    ores_ref, cnt_ref, rank_ref, ocnt_ref, orank_ref,
    acts_v, cot_v, res_v, rk_ref, rp_ref, mt_ref, msend, mrecv,
    sent, psum, tsend, trecv, usend, urecv, osend, orecv, okeep,
    in_sem, s_sem, g_sem, mr_sem, sr_sem, tr_sem, zr_sem, fr_sem,
):
    n_in, n_out, steps, scale, region, width = dims
    rows, cols = acts_v.shape[2], cot_v.shape[2]
    cpr = cols // width
    rpr = region // cpr
    halves = region // LANES
    chunk = 2 * LANES
    rpc = chunk // rpr
    n_z = n_in // 2
    me = lax.axis_index("inner")
    pod = lax.axis_index("outer")
    core = lax.rem(me, 2)
    z = lax.div(me, 2)
    partner = me + 1 - 2 * core
    OVER_Z, KEPT, HAND, MASK, SHARE, TOTAL, GATHER_Z, GATHER_O = range(8)

    def outer(d):
        return lax.rem(pod + d, n_out)

    def flip(m):
        v, bit = z, 1
        while bit <= m:
            if m & bit:
                v = v + bit - 2 * bit * lax.rem(lax.div(z, bit), 2)
            bit *= 2
        return v

    def same_core(zz):
        return 2 * zz + core

    far_first = list(range(n_z - 1, 0, -1))

    def remote(src, dst, ssem, rsem, **device):
        return pltpu.make_async_remote_copy(
            src_ref=src, dst_ref=dst, send_sem=ssem, recv_sem=rsem,
            device_id=device, device_id_type=pl.DeviceIdType.MESH,
        )

    def send(phase, src, dst, rsem, **device):
        remote(src, dst, s_sem.at[phase], rsem, **device).start()

    def arrived(ref, rsem):
        remote(ref, ref, s_sem.at[0], rsem, inner=partner).wait_recv()

    def left(phase, ref):
        remote(ref, ref, s_sem.at[phase], g_sem.at[0], inner=partner).wait_send()

    barrier = pltpu.get_barrier_semaphore()
    for m in far_first:
        pl.semaphore_signal(barrier, inc=1, device_id={"inner": same_core(flip(m))}, device_id_type=pl.DeviceIdType.MESH)
    for d in range(1, n_out):
        pl.semaphore_signal(barrier, inc=1, device_id={"outer": outer(d)}, device_id_type=pl.DeviceIdType.MESH)
    pl.semaphore_signal(barrier, inc=1, device_id={"inner": partner}, device_id_type=pl.DeviceIdType.MESH)

    small = [
        pltpu.make_async_copy(src, dst, in_sem.at[k])
        for k, (src, dst) in enumerate(
            ((rank_hbm, rank_ref), (cnt_hbm, cnt_ref), (orank_hbm, orank_ref), (ocnt_hbm, ocnt_ref), (ores_hbm, ores_ref))
        )
    ]
    for copy in small:
        copy.start()

    def fetch(s):
        pltpu.make_async_copy(acts_hbm.at[s], acts_v.at[s], in_sem.at[6 + s]).start()
        pltpu.make_async_copy(cot_hbm.at[s], cot_v.at[s], in_sem.at[6 + s]).start()

    fetch(0)
    res_load = pltpu.make_async_copy(res_hbm, res_v, in_sem.at[5])
    res_load.start()

    def loaded(s):
        both = acts_v.at[0:2]
        pltpu.make_async_copy(both, both, in_sem.at[6 + s]).wait()

    rk_ref[...] = jnp.zeros(rk_ref.shape, F32)
    msend[...] = jnp.zeros(msend.shape, F32)
    for copy in small:
        copy.wait()
    for s in range(1, steps):
        fetch(s)
    for s in range(steps):
        for j in range(n_in):
            row = rank_ref[s : s + 1, j * region : (j + 1) * region]
            rk_ref[s * n_in + j : s * n_in + j + 1, :] = jnp.where(row < cnt_ref[s : s + 1, j : j + 1], 1.0, 0.0)
    later = jnp.zeros((1, region), F32)
    for s in reversed(range(steps)):
        later = jnp.where(orank_ref[s : s + 1, :] < ocnt_ref[0:1, s : s + 1], 1.0, later)
        rk_ref[steps * n_in + s : steps * n_in + s + 1, :] = later
    old = lax.broadcasted_iota(jnp.int32, (region, region), 0)
    new = lax.broadcasted_iota(jnp.int32, (region, region), 1)
    shift = rpr.bit_length() - 1
    perm = jnp.where(old == (new & (rpr - 1)) * cpr + (new >> shift), 1.0, 0.0).astype(BF16)
    rp = jnp.dot(rk_ref[...].astype(BF16), perm, preferred_element_type=F32)
    rp_ref[...] = rp

    def eye(n):
        return jnp.where(
            lax.broadcasted_iota(jnp.int32, (n, LANES), 0) == lax.broadcasted_iota(jnp.int32, (n, LANES), 1), 1.0, 0.0
        ).astype(BF16)

    def turned(values):
        return lax.dot_general(
            values.astype(BF16), eye(values.shape[0]), (((0,), (0,)), ((), ())), preferred_element_type=F32
        ).astype(BF16)

    def spread(table, index, n):
        pick = jnp.where(lax.broadcasted_iota(jnp.int32, (LANES, n), 0) == index, 1.0, 0.0).astype(BF16)
        return jnp.dot(table, pick, preferred_element_type=F32)

    for s in range(steps):
        for h in range(halves):
            msend[s * halves + h : s * halves + h + 1, :] = rp_ref[
                steps * n_in + s : steps * n_in + s + 1, h * LANES : (h + 1) * LANES
            ]
    mt_ref[...] = turned(rp)

    def greet():
        pl.semaphore_wait(barrier, n_z - 1 + n_out)
        for m in far_first:
            send(MASK, msend, mrecv.at[z], mr_sem.at[z], inner=same_core(flip(m)))

    def share(s, zz):
        send(SHARE, sent.at[s, 2 * zz + 1 - core], psum.at[s, zz], sr_sem.at[s], inner=partner)

    met = False
    waiting = []
    for s in range(steps):
        if not met and (0, 1) == (s, -1):
            greet()
            met = True
        loaded(s)
        if s == 0:
            res_load.wait()
        for q in range(rows // chunk):
            g = lax.dot_general(
                acts_v[s, :, q * chunk : (q + 1) * chunk], cot_v[s], (((0,), (0,)), ((), ())),
                preferred_element_type=F32,
            ) * scale
            for half in range(rpc):
                j = q * rpc + half
                chosen = spread(mt_ref[...], s * n_in + j, width) > 0.5
                for c in range(cpr):
                    where_at = pl.ds(region * j + c, rpr, stride=cpr)
                    acc = res_v[where_at, :] + g[half * rpr : (half + 1) * rpr, c * width : (c + 1) * width]
                    take = chosen[c * rpr : (c + 1) * rpr]
                    (resid_ref if s == steps - 1 else res_v)[where_at, :] = jnp.where(take, 0.0, acc)
                    sent[s, j, c * rpr : (c + 1) * rpr] = jnp.where(take, acc, 0.0).astype(BF16)
            waiting += [(s, zz) for zz in range(q * rpc // 2, (q + 1) * rpc // 2)]
            if not met and (0, 1) == (s, q):
                greet()
                met = True
            if met:
                for pair in waiting:
                    share(*pair)
                waiting = []

    for s in range(steps):
        arrived(psum.at[s], sr_sem.at[s])

    def passed(m, s):
        if m == 0:
            return spread(mt_ref[...], steps * n_in + s, width) > 0.5
        rows_of = mrecv[flip(m)].astype(BF16)
        parts = []
        for h in range(halves):
            pick = jnp.where(lax.broadcasted_iota(jnp.int32, (16, width), 0) == s * halves + h, 1.0, 0.0).astype(BF16)
            parts.append(lax.dot_general(rows_of, pick, (((0,), (0,)), ((), ())), preferred_element_type=F32))
        return jnp.concatenate(parts, axis=0) > 0.5

    def chip_sum(m, s):
        part = sent[s, same_core(flip(m))].astype(F32) + psum[s, flip(m)].astype(F32)
        if m == 0 and s == 0:
            part = part + jnp.concatenate([ores_ref[pl.ds(c, rpr, stride=cpr), :] for c in range(cpr)], axis=0)
        return part

    def send_total(m):
        zz = flip(m)
        t = jnp.zeros((region, width), F32)
        for s in range(steps):
            t = t + jnp.where(passed(m, s), chip_sum(m, s), 0.0)
        for q in range(n_out):
            tsend[zz, q] = t[q * rpr : (q + 1) * rpr].astype(BF16)
        for d in range(1, n_out):
            send(TOTAL, tsend.at[zz, outer(d)], trecv.at[zz, pod], tr_sem.at[zz], outer=outer(d))

    def keep(m):
        o = jnp.zeros((region, width), F32)
        for s in range(steps):
            o = o + jnp.where(passed(m, s), 0.0, chip_sum(m, s))
        return o

    def send_kept(m):
        osend[flip(m)] = keep(m).astype(BF16)
        send(KEPT, osend.at[flip(m)], orecv.at[z], g_sem.at[KEPT], inner=same_core(flip(m)))

    send_total(0)
    for m in (1, 2, 3):
        arrived(mrecv.at[flip(m)], mr_sem.at[flip(m)])
        send_total(m)
    for m in (3, 1):
        send_kept(m)
    okeep[...] = keep(0)

    for m in (1, 2, 3) + (0,):
        zz = flip(m)
        arrived(trecv.at[zz, 0 : n_out - 1], tr_sem.at[zz])
        total = tsend[zz, pod].astype(F32)
        for d in range(1, n_out):
            total = total + trecv[zz, outer(d)].astype(F32)
        if m:
            usend[zz] = total.astype(BF16)
            send(OVER_Z, usend.at[zz], urecv.at[z], g_sem.at[OVER_Z], inner=same_core(zz))
    arrived(urecv.at[0 : n_z - 1], g_sem.at[OVER_Z])
    for m in far_first:
        total = total + urecv[flip(m)].astype(F32)
    own = ag.at[pod, z, core]
    own[...] = (-step_size * total).astype(BF16)

    def forward(m):
        zz = flip(m)
        piece = ag.at[pod, zz, core]
        for d in range(1, n_out):
            send(GATHER_O, piece, piece, fr_sem.at[zz], outer=outer(d))

    def hand_over(q, m):
        piece = ag.at[q, flip(m), core]
        send(HAND, piece, piece, g_sem.at[HAND], inner=partner)

    for m in far_first:
        send(GATHER_Z, own, own, zr_sem.at[z], inner=same_core(flip(m)))
    forward(0)
    hand_over(pod, 0)
    for m in (2,):
        send_kept(m)

    for m in reversed(far_first):
        arrived(ag.at[pod, flip(m), core], zr_sem.at[flip(m)])
        forward(m)
        hand_over(pod, m)
    for m in range(n_z):
        arrived(ag.at[0 : n_out - 1, flip(m), core], fr_sem.at[flip(m)])
        for d in range(1, n_out):
            hand_over(outer(d), m)
    arrived(orecv.at[0 : n_z - 1], g_sem.at[KEPT])
    kept = okeep[...]
    for m in far_first:
        kept = kept + orecv[flip(m)].astype(F32)
    for c in range(cpr):
        nores_ref[pl.ds(c, rpr, stride=cpr), :] = kept[c * rpr : (c + 1) * rpr]

    arrived(ag.at[:, :, 1 - core], g_sem.at[HAND])
    left(MASK, mrecv.at[0 : n_z - 1])
    left(SHARE, psum)
    left(TOTAL, trecv.at[:, 0 : n_out - 1])
    left(OVER_Z, urecv.at[0 : n_z - 1])
    left(KEPT, orecv.at[0 : n_z - 1])
    left(GATHER_Z, urecv.at[0 : n_z - 1])
    left(GATHER_O, trecv.at[:, 0 : n_out - 1])
    left(HAND, trecv)


def hand_out(pieces, *arrays):
    n = len(arrays)
    pods, rows, width = pieces.shape

    def kernel(*refs):
        src, dst, sems = refs[: n + 1], refs[n + 1 : 2 * n + 2], refs[2 * n + 2]
        copies = [pltpu.make_async_copy(src[k], dst[k], sems.at[k]) for k in range(1, n + 1)]
        copies += [
            pltpu.make_async_copy(src[0].at[q], dst[0].at[:, q * width : (q + 1) * width], sems.at[n + 1 + q])
            for q in range(pods)
        ]
        for copy in copies:
            copy.start()
        for copy in copies:
            copy.wait()

    return pl.pallas_call(
        kernel,
        out_shape=(jax.ShapeDtypeStruct((rows, pods * width), pieces.dtype),)
        + tuple(jax.ShapeDtypeStruct(a.shape, a.dtype) for a in arrays),
        in_specs=[pl.BlockSpec(memory_space=pltpu.VMEM)] * (n + 1),
        out_specs=tuple([pl.BlockSpec(memory_space=pltpu.HBM)] * (n + 1)),
        scratch_shapes=[pltpu.SemaphoreType.DMA((n + 1 + pods,))],
        compiler_params=pltpu.CompilerParams(vmem_limit_bytes=4 << 20),
    )(pieces, *arrays)


def fits(owners, pods, steps, rows, cols, blocks, width, region):
    if width != LANES or region % LANES or region > 256 or cols % width or owners % 4:
        return False
    cpr = cols // width
    rpr = region // cpr
    n_z = owners // 2
    return (
        cpr == pods and cpr * rpr == region and rpr % 16 == 0 and 2 * rpr == LANES
        and rows % LANES == 0 and n_z & (n_z - 1) == 0
        and rpr * owners == rows and steps * (owners + 1) <= LANES and steps * (region // LANES) <= 8
    )


def per_device_fused(acts, cotangent, residual, owner_residual, in_count, in_rank, out_count, out_rank):
    n_in = lax.axis_size("inner")
    n_out = lax.axis_size("outer")
    steps, tokens, rows = acts.shape[1:]
    cols = cotangent.shape[3]
    blocks, width = residual.shape[1:]
    region = blocks // n_in
    if not fits(n_in, n_out, steps, rows, cols, blocks, width, region):
        return per_device(acts, cotangent, residual, owner_residual, in_count, in_rank, out_count, out_rank)
    scale = 1.0 / math.sqrt(tokens * n_in)
    rpr = region // n_out
    n_z = n_in // 2
    n_rk = -(-steps * (n_in + 1) // 16) * 16
    vmem = pl.BlockSpec(memory_space=pltpu.VMEM)
    anywhere = pl.BlockSpec(memory_space=pltpu.HBM)
    dma = pltpu.SemaphoreType.DMA
    pieces, resid, oresid = pl.pallas_call(
        functools.partial(fused_kernel, (n_in, n_out, steps, scale, region, width)),
        out_shape=(
            jax.ShapeDtypeStruct((n_out, n_z, 2, rpr, width), BF16),
            jax.ShapeDtypeStruct((blocks, width), F32),
            jax.ShapeDtypeStruct((region, width), F32),
        ),
        in_specs=[anywhere] * 8,
        out_specs=(vmem, vmem, vmem),
        scratch_shapes=[
            pltpu.VMEM((region, width), F32),
            pltpu.VMEM((steps, n_in), jnp.int32),
            pltpu.VMEM((steps, blocks), jnp.int32),
            pltpu.VMEM((1, steps), jnp.int32),
            pltpu.VMEM((steps, region), jnp.int32),
            pltpu.VMEM((steps, tokens, rows), BF16),
            pltpu.VMEM((steps, tokens, cols), BF16),
            pltpu.VMEM((blocks, width), F32),
            pltpu.VMEM((n_rk, region), F32),
            pltpu.VMEM((n_rk, region), F32),
            pltpu.VMEM((region, LANES), BF16),
            pltpu.VMEM((16, LANES), F32),
            pltpu.VMEM((n_z, 16, LANES), F32),
            pltpu.VMEM((steps, n_in, region, width), BF16),
            pltpu.VMEM((steps, n_z, region, width), BF16),
            pltpu.VMEM((n_z, n_out, rpr, width), BF16),
            pltpu.VMEM((n_z, n_out, rpr, width), BF16),
            pltpu.VMEM((n_z, rpr, width), BF16),
            pltpu.VMEM((n_z, rpr, width), BF16),
            pltpu.VMEM((n_z, region, width), BF16),
            pltpu.VMEM((n_z, region, width), BF16),
            pltpu.VMEM((region, width), F32),
            dma((6 + steps,)),
            dma((8,)),
            dma((3,)),
            dma((n_z,)),
            dma((steps,)),
            dma((n_z,)),
            dma((n_z,)),
            dma((n_z,)),
        ],
        compiler_params=pltpu.CompilerParams(collective_id=0, has_side_effects=True, vmem_limit_bytes=48 << 20),
    )(*(
        pltpu.with_memory_space_constraint(a, pltpu.HBM)
        for a in (
            acts[0], cotangent[0], residual[0], owner_residual[0], in_count[0], in_rank[0], out_count, out_rank[0]
        )
    ))
    applied, resid, oresid = hand_out(pieces.reshape(n_out, rows, width), resid, oresid)
    return applied, resid[None], oresid[None]


def solution(mesh):
    return jax.shard_map(
        per_device_fused,
        mesh=mesh,
        in_specs=(
            P(("outer", "inner"), None, None, None),
            P(("outer", "inner"), None, None, None),
            P(("outer", "inner"), None, None),
            P(("outer", "inner"), None, None),
            P(("outer", "inner"), None, None),
            P(("outer", "inner"), None, None),
            P(("outer", "inner"), None),
            P(("outer", "inner"), None, None),
        ),
        out_specs=(P(), P(("outer", "inner"), None, None), P(("outer", "inner"), None, None)),
        check_vma=False,
    )
```

```python
import functools
import math

import jax
import jax.numpy as jnp
from jax import lax
from jax.experimental import pallas as pl
from jax.experimental.pallas import tpu as pltpu
from jax.sharding import PartitionSpec as P

step_size = 0.0625


def select_blocks(resid, grad, ranks_flat, counts, owners, region, width):
    blocks = resid.shape[0]
    accum = (resid + grad.reshape(blocks, width)).reshape(owners, region, width)
    ranks = ranks_flat.reshape(owners, region)
    chosen = (ranks < counts[:, None])[..., None]
    new_resid = jnp.where(chosen, jnp.float32(0.0), accum).reshape(blocks, width)
    return (accum, ranks, chosen, new_resid)


def pack_slots(accum, ranks, counts, slots, region):
    order = lax.iota(jnp.int32, slots)
    picks = (ranks[:, None, :] == order[None, :, None]) & (
        order[None, :, None] < counts[:, None, None]
    )
    picks_f = picks.astype(jnp.float32)
    places = lax.iota(jnp.int32, region).astype(jnp.float32)
    packed = jnp.einsum("nkr,nrd->nkd", picks_f, accum, precision=lax.Precision.HIGHEST)
    where_at = jnp.einsum("nkr,r->nk", picks_f, places, precision=lax.Precision.HIGHEST)
    return (packed, where_at)


def unpack_slots(arrived, spots, region, width):
    places = lax.iota(jnp.int32, region).astype(jnp.float32)
    placed = (spots.reshape(-1)[:, None] == places[None, :]).astype(jnp.float32)
    return jnp.einsum(
        "mr,md->rd", placed, arrived.reshape(-1, width), precision=lax.Precision.HIGHEST
    )


def owner_section(pod_sum, oresid, ranks_out, count_out):
    owner_acc = pod_sum + oresid
    passed = (ranks_out < count_out)[:, None]
    outgoing = jnp.where(passed, owner_acc, jnp.float32(0.0))
    kept = jnp.where(passed, jnp.float32(0.0), owner_acc)
    return (outgoing, kept)


def per_device(acts, cotangent, residual, owner_residual, in_count, in_rank, out_count, out_rank):
    owners = lax.axis_size("inner")
    steps = acts.shape[1]
    tokens = acts.shape[2]
    rows = acts.shape[3]
    cols = cotangent.shape[3]
    blocks = residual.shape[1]
    width = residual.shape[2]
    region = blocks // owners
    slots = max(1, region // 2)
    scale = 1.0 / math.sqrt(tokens * owners)
    resid = residual[0]
    oresid = owner_residual[0]
    crosses = []
    packs = []
    spots_all = []
    for step in range(steps):
        grad = (
            jnp.einsum(
                "tr,tc->rc", acts[0, step], cotangent[0, step], preferred_element_type=jnp.float32
            )
            * scale
        )
        counts = in_count[0, step]
        accum, ranks, chosen, resid = select_blocks(
            resid, grad, in_rank[0, step], counts, owners, region, width
        )
        packed, where_at = pack_slots(accum, ranks, counts, slots, region)
        packs.append(packed)
        spots_all.append(where_at)
    arrived, spots = (
        lax.all_to_all(
            jnp.concatenate(packs, axis=1), "inner", split_axis=0, concat_axis=0, tiled=True
        ),
        lax.all_to_all(
            jnp.concatenate(spots_all, axis=1), "inner", split_axis=0, concat_axis=0, tiled=True
        ),
    )
    outgoings = []
    for step in range(steps):
        pod_sum = unpack_slots(
            arrived[:, step * slots : (step + 1) * slots],
            spots[:, step * slots : (step + 1) * slots],
            region,
            width,
        )
        outgoing, oresid = owner_section(pod_sum, oresid, out_rank[0, step], out_count[0, step])
        outgoings.append(outgoing)
    summed = lax.psum(jnp.stack(outgoings), "outer")
    for step in range(steps):
        crosses.append(summed[step])
    deltas = []
    for cross in crosses:
        delta = cross.astype(jnp.bfloat16)
        deltas.append(lax.all_gather(delta, "inner", axis=0, tiled=True))
    total = deltas[0].astype(jnp.float32)
    for later in deltas[1:]:
        total = total + later.astype(jnp.float32)
    applied = (-step_size * total).astype(jnp.bfloat16)
    return (applied.reshape(rows, cols), resid[None], oresid[None])


LANES = 128
F32 = jnp.float32
BF16 = jnp.bfloat16


def fused_kernel(
    dims,
    acts_hbm, cot_hbm, res_hbm, ores_hbm, cnt_hbm, rank_hbm, ocnt_hbm, orank_hbm,
    ag, resid_ref, nores_ref,
    ores_ref, cnt_ref, rank_ref, ocnt_ref, orank_ref,
    acts_v, cot_v, res_v, rk_ref, rp_ref, mt_ref, msend, mrecv,
    sent, psum, tsend, trecv, usend, urecv, osend, orecv, okeep,
    sent_bytes, in_sem, s_sem, g_sem, mr_sem, sr_sem, tr_sem, zr_sem, fr_sem,
):
    n_in, n_out, steps, scale, region, width = dims
    rows, cols = acts_v.shape[2], cot_v.shape[2]
    cpr = cols // width
    rpr = region // cpr
    halves = region // LANES
    chunk = 2 * LANES
    rpc = chunk // rpr
    n_z = n_in // 2
    me = lax.axis_index("inner")
    pod = lax.axis_index("outer")
    core = lax.rem(me, 2)
    z = lax.div(me, 2)
    partner = me + 1 - 2 * core
    OVER_Z, KEPT, HAND, MASK, SHARE, TOTAL, GATHER_Z, GATHER_O = range(8)

    def flipped(at, m):
        v, bit = at, 1
        while bit <= m:
            if m & bit:
                v = v + bit - 2 * bit * lax.rem(lax.div(at, bit), 2)
            bit *= 2
        return v

    def flip(m):
        return flipped(z, m)

    def outer(d):
        return flipped(pod, d)

    def same_core(zz):
        return 2 * zz + core

    far_first = list(range(n_z - 1, 0, -1))
    far_pods = list(range(n_out - 1, 0, -1))

    def remote(src, dst, ssem, rsem, **device):
        return pltpu.make_async_remote_copy(
            src_ref=src, dst_ref=dst, send_sem=ssem, recv_sem=rsem,
            device_id=device, device_id_type=pl.DeviceIdType.MESH,
        )

    def send(phase, src, dst, rsem, **device):
        remote(src, dst, s_sem.at[0], rsem, **device).start()

    def arrived(ref, rsem):
        remote(ref, ref, s_sem.at[0], rsem, inner=partner).wait_recv()

    def left(phase, ref):
        remote(ref, ref, s_sem.at[0], g_sem.at[0], inner=partner).wait_send()

    barrier = pltpu.get_barrier_semaphore()
    for m in far_first:
        pl.semaphore_signal(barrier, inc=1, device_id={"inner": same_core(flip(m))}, device_id_type=pl.DeviceIdType.MESH)
    for d in far_pods:
        pl.semaphore_signal(barrier, inc=1, device_id={"outer": outer(d)}, device_id_type=pl.DeviceIdType.MESH)
        pl.semaphore_signal(barrier, inc=1, device_id={"outer": outer(d), "inner": partner}, device_id_type=pl.DeviceIdType.MESH)
    pl.semaphore_signal(barrier, inc=1, device_id={"inner": partner}, device_id_type=pl.DeviceIdType.MESH)

    small = [
        pltpu.make_async_copy(src, dst, in_sem.at[k])
        for k, (src, dst) in enumerate(
            ((rank_hbm, rank_ref), (cnt_hbm, cnt_ref), (orank_hbm, orank_ref), (ocnt_hbm, ocnt_ref), (ores_hbm, ores_ref))
        )
    ]
    for copy in small:
        copy.start()

    def fetch(s):
        pltpu.make_async_copy(acts_hbm.at[s], acts_v.at[s], in_sem.at[6 + s]).start()
        pltpu.make_async_copy(cot_hbm.at[s], cot_v.at[s], in_sem.at[6 + s]).start()

    fetch(0)
    res_load = pltpu.make_async_copy(res_hbm, res_v, in_sem.at[5])
    res_load.start()

    def loaded(s):
        both = acts_v.at[0:2]
        pltpu.make_async_copy(both, both, in_sem.at[6 + s]).wait()

    rk_ref[...] = jnp.zeros(rk_ref.shape, F32)
    msend[...] = jnp.zeros(msend.shape, F32)
    for copy in small:
        copy.wait()
    for s in range(1, steps):
        fetch(s)
    for s in range(steps):
        for j in range(n_in):
            row = rank_ref[s : s + 1, j * region : (j + 1) * region]
            rk_ref[s * n_in + j : s * n_in + j + 1, :] = jnp.where(row < cnt_ref[s : s + 1, j : j + 1], 1.0, 0.0)
    later = jnp.zeros((1, region), F32)
    for s in reversed(range(steps)):
        later = jnp.where(orank_ref[s : s + 1, :] < ocnt_ref[0:1, s : s + 1], 1.0, later)
        rk_ref[steps * n_in + s : steps * n_in + s + 1, :] = later
    old = lax.broadcasted_iota(jnp.int32, (region, region), 0)
    new = lax.broadcasted_iota(jnp.int32, (region, region), 1)
    shift = rpr.bit_length() - 1
    perm = jnp.where(old == (new & (rpr - 1)) * cpr + (new >> shift), 1.0, 0.0).astype(BF16)
    rp = jnp.dot(rk_ref[...].astype(BF16), perm, preferred_element_type=F32)
    rp_ref[...] = rp

    def eye(n):
        return jnp.where(
            lax.broadcasted_iota(jnp.int32, (n, LANES), 0) == lax.broadcasted_iota(jnp.int32, (n, LANES), 1), 1.0, 0.0
        ).astype(BF16)

    def turned(values):
        return lax.dot_general(
            values.astype(BF16), eye(values.shape[0]), (((0,), (0,)), ((), ())), preferred_element_type=F32
        ).astype(BF16)

    def spread(table, index, n):
        pick = jnp.where(lax.broadcasted_iota(jnp.int32, (LANES, n), 0) == index, 1.0, 0.0).astype(BF16)
        return jnp.dot(table, pick, preferred_element_type=F32)

    for s in range(steps):
        for h in range(halves):
            msend[s * halves + h : s * halves + h + 1, :] = rp_ref[
                steps * n_in + s : steps * n_in + s + 1, h * LANES : (h + 1) * LANES
            ]
    mt_ref[...] = turned(rp)

    def greet():
        pl.semaphore_wait(barrier, n_z - 1 + n_out + n_out - 1)
        for m in far_first:
            send(MASK, msend, mrecv.at[z], mr_sem.at[m - 1], inner=same_core(flip(m)))

    def share(s, zz):
        send(SHARE, sent.at[s, 2 * zz + 1 - core], psum.at[s, zz], sr_sem.at[s], inner=partner)

    met = False
    waiting = []
    for s in range(steps):
        loaded(s)
        if s == 0:
            res_load.wait()
        for q in range(rows // chunk):
            g = lax.dot_general(
                acts_v[s, :, q * chunk : (q + 1) * chunk], cot_v[s], (((0,), (0,)), ((), ())),
                preferred_element_type=F32,
            ) * scale
            for half in range(rpc):
                j = q * rpc + half
                chosen = spread(mt_ref[...], s * n_in + j, width) > 0.5
                for c in range(cpr):
                    where_at = pl.ds(region * j + c, rpr, stride=cpr)
                    acc = res_v[where_at, :] + g[half * rpr : (half + 1) * rpr, c * width : (c + 1) * width]
                    take = chosen[c * rpr : (c + 1) * rpr]
                    (resid_ref if s == steps - 1 else res_v)[where_at, :] = jnp.where(take, 0.0, acc)
                    sent[s, j, c * rpr : (c + 1) * rpr] = jnp.where(take, acc, 0.0).astype(BF16)
            waiting += [(s, zz) for zz in range(q * rpc // 2, (q + 1) * rpc // 2)]
            if s == 0 and q == rows // chunk - 1:
                greet()
                met = True
            if met:
                for pair in waiting:
                    share(*pair)
                waiting = []

    for s in range(steps):
        arrived(psum.at[s], sr_sem.at[s])

    def passed(m, s):
        if m == 0:
            return spread(mt_ref[...], steps * n_in + s, width) > 0.5
        rows_of = mrecv[flip(m)].astype(BF16)
        parts = []
        for h in range(halves):
            pick = jnp.where(lax.broadcasted_iota(jnp.int32, (16, width), 0) == s * halves + h, 1.0, 0.0).astype(BF16)
            parts.append(lax.dot_general(rows_of, pick, (((0,), (0,)), ((), ())), preferred_element_type=F32))
        return jnp.concatenate(parts, axis=0) > 0.5

    def chip_sum(m, s):
        part = sent[s, same_core(flip(m))].astype(F32) + psum[s, flip(m)].astype(F32)
        if m == 0 and s == 0:
            part = part + jnp.concatenate([ores_ref[pl.ds(c, rpr, stride=cpr), :] for c in range(cpr)], axis=0)
        return part

    def send_total(m):
        zz = flip(m)
        t = jnp.zeros((region, width), F32)
        for s in range(steps):
            t = t + jnp.where(passed(m, s), chip_sum(m, s), 0.0)
        for q in range(n_out):
            tsend[zz, q] = t[q * rpr : (q + 1) * rpr].astype(BF16)
        for d in far_pods:
            send(TOTAL, tsend.at[zz, outer(d)], trecv.at[zz, pod], tr_sem.at[m], outer=outer(d))

    def keep(m):
        o = jnp.zeros((region, width), F32)
        for s in range(steps):
            o = o + jnp.where(passed(m, s), 0.0, chip_sum(m, s))
        return o

    def send_kept(m):
        osend[flip(m)] = keep(m).astype(BF16)
        send(KEPT, osend.at[flip(m)], orecv.at[z], g_sem.at[KEPT], inner=same_core(flip(m)))

    send_total(0)
    for m in reversed(far_first):
        arrived(mrecv.at[flip(m)], mr_sem.at[m - 1])
        send_total(m)
    late = n_z // 2
    for m in far_first:
        if m != late:
            send_kept(m)
    okeep[...] = keep(0)

    for m in far_first[::-1] + [0]:
        zz = flip(m)
        arrived(trecv.at[zz, 0 : n_out - 1], tr_sem.at[m])
        total = tsend[zz, pod].astype(F32)
        for d in far_pods:
            total = total + trecv[zz, outer(d)].astype(F32)
        if m:
            usend[zz] = total.astype(BF16)
            send(OVER_Z, usend.at[zz], urecv.at[z], g_sem.at[OVER_Z], inner=same_core(zz))
    arrived(urecv.at[0 : n_z - 1], g_sem.at[OVER_Z])
    for m in far_first:
        total = total + urecv[flip(m)].astype(F32)
    own = ag.at[pod, z, core]
    own[...] = (-step_size * total).astype(BF16)

    def forward(m):
        zz = flip(m)
        piece = ag.at[pod, zz, core]
        for d in far_pods:
            send(GATHER_O, piece, piece, fr_sem.at[m], outer=outer(d))
            if m == n_z - 1:
                send(GATHER_O, piece, piece, g_sem.at[HAND], outer=outer(d), inner=partner)

    def hand_over(q, m):
        piece = ag.at[q, flip(m), core]
        send(HAND, piece, piece, g_sem.at[HAND], inner=partner)

    for m in far_first:
        send(GATHER_Z, own, own, zr_sem.at[m - 1], inner=same_core(flip(m)))
    forward(0)
    hand_over(pod, 0)
    send_kept(late)

    for m in reversed(far_first):
        arrived(ag.at[pod, flip(m), core], zr_sem.at[m - 1])
        forward(m)
        hand_over(pod, m)
    for m in range(n_z):
        arrived(ag.at[0 : n_out - 1, flip(m), core], fr_sem.at[m])
        for d in far_pods:
            if m < n_z - 1:
                hand_over(outer(d), m)
    arrived(orecv.at[0 : n_z - 1], g_sem.at[KEPT])
    kept = okeep[...]
    for m in far_first:
        kept = kept + orecv[flip(m)].astype(F32)
    for c in range(cpr):
        nores_ref[pl.ds(c, rpr, stride=cpr), :] = kept[c * rpr : (c + 1) * rpr]

    arrived(ag.at[:, :, 1 - core], g_sem.at[HAND])
    left(0, sent_bytes)


def hand_out(pieces, *arrays):
    n = len(arrays)
    pods, rows, width = pieces.shape

    def kernel(*refs):
        src, dst, sems = refs[: n + 1], refs[n + 1 : 2 * n + 2], refs[2 * n + 2]
        copies = [pltpu.make_async_copy(src[k], dst[k], sems.at[k]) for k in range(1, n + 1)]
        copies += [
            pltpu.make_async_copy(src[0].at[q], dst[0].at[:, q * width : (q + 1) * width], sems.at[n + 1 + q])
            for q in range(pods)
        ]
        for copy in copies:
            copy.start()
        for copy in copies:
            copy.wait()

    return pl.pallas_call(
        kernel,
        out_shape=(jax.ShapeDtypeStruct((rows, pods * width), pieces.dtype),)
        + tuple(jax.ShapeDtypeStruct(a.shape, a.dtype) for a in arrays),
        in_specs=[pl.BlockSpec(memory_space=pltpu.VMEM)] * (n + 1),
        out_specs=tuple([pl.BlockSpec(memory_space=pltpu.HBM)] * (n + 1)),
        scratch_shapes=[pltpu.SemaphoreType.DMA((n + 1 + pods,))],
        compiler_params=pltpu.CompilerParams(vmem_limit_bytes=4 << 20),
    )(pieces, *arrays)


def fits(owners, pods, steps, rows, cols, blocks, width, region):
    if width != LANES or region % LANES or region > 256 or cols % width or owners % 4:
        return False
    cpr = cols // width
    rpr = region // cpr
    n_z = owners // 2
    return (
        cpr == pods and steps >= 2 and rows == cols and cpr * rpr == region and rpr % 16 == 0 and 2 * rpr == LANES
        and rows % (2 * LANES) == 0 and n_z & (n_z - 1) == 0 and pods & (pods - 1) == 0
        and rpr * owners == rows and steps * (owners + 1) <= LANES and steps * (region // LANES) <= 8
    )


def per_device_fused(acts, cotangent, residual, owner_residual, in_count, in_rank, out_count, out_rank):
    n_in = lax.axis_size("inner")
    n_out = lax.axis_size("outer")
    steps, tokens, rows = acts.shape[1:]
    cols = cotangent.shape[3]
    blocks, width = residual.shape[1:]
    region = blocks // n_in
    if not fits(n_in, n_out, steps, rows, cols, blocks, width, region):
        return per_device(acts, cotangent, residual, owner_residual, in_count, in_rank, out_count, out_rank)
    scale = 1.0 / math.sqrt(tokens * n_in)
    rpr = region // n_out
    n_z = n_in // 2
    n_rk = -(-steps * (n_in + 1) // 16) * 16
    piece = rpr // 2
    n_sent = (n_z - 1) * (16 + 2 * piece + region // 2) + steps * n_z * region // 2
    n_sent += 2 * n_z * (n_out - 1) * piece + n_z * n_out * piece
    vmem = pl.BlockSpec(memory_space=pltpu.VMEM)
    anywhere = pl.BlockSpec(memory_space=pltpu.HBM)
    dma = pltpu.SemaphoreType.DMA
    pieces, resid, oresid = pl.pallas_call(
        functools.partial(fused_kernel, (n_in, n_out, steps, scale, region, width)),
        out_shape=(
            jax.ShapeDtypeStruct((n_out, n_z, 2, rpr, width), BF16),
            jax.ShapeDtypeStruct((blocks, width), F32),
            jax.ShapeDtypeStruct((region, width), F32),
        ),
        in_specs=[anywhere] * 8,
        out_specs=(vmem, vmem, vmem),
        scratch_shapes=[
            pltpu.VMEM((region, width), F32),
            pltpu.VMEM((steps, n_in), jnp.int32),
            pltpu.VMEM((steps, blocks), jnp.int32),
            pltpu.VMEM((1, steps), jnp.int32),
            pltpu.VMEM((steps, region), jnp.int32),
            pltpu.VMEM((steps, tokens, rows), BF16),
            pltpu.VMEM((steps, tokens, cols), BF16),
            pltpu.VMEM((blocks, width), F32),
            pltpu.VMEM((n_rk, region), F32),
            pltpu.VMEM((n_rk, region), F32),
            pltpu.VMEM((region, LANES), BF16),
            pltpu.VMEM((16, LANES), F32),
            pltpu.VMEM((n_z, 16, LANES), F32),
            pltpu.VMEM((steps, n_in, region, width), BF16),
            pltpu.VMEM((steps, n_z, region, width), BF16),
            pltpu.VMEM((n_z, n_out, rpr, width), BF16),
            pltpu.VMEM((n_z, n_out, rpr, width), BF16),
            pltpu.VMEM((n_z, rpr, width), BF16),
            pltpu.VMEM((n_z, rpr, width), BF16),
            pltpu.VMEM((n_z, region, width), BF16),
            pltpu.VMEM((n_z, region, width), BF16),
            pltpu.VMEM((region, width), F32),
            pltpu.VMEM((n_sent, LANES), F32),
            dma((6 + steps,)),
            dma((1,)),
            dma((3,)),
            dma((n_z - 1,)),
            dma((steps,)),
            dma((n_z,)),
            dma((n_z - 1,)),
            dma((n_z,)),
        ],
        compiler_params=pltpu.CompilerParams(collective_id=0, has_side_effects=True, vmem_limit_bytes=48 << 20),
    )(*(
        pltpu.with_memory_space_constraint(a, pltpu.HBM)
        for a in (
            acts[0], cotangent[0], residual[0], owner_residual[0], in_count[0], in_rank[0], out_count, out_rank[0]
        )
    ))
    applied, resid, oresid = hand_out(pieces.reshape(n_out, rows, width), resid, oresid)
    return applied, resid[None], oresid[None]


def solution(mesh):
    return jax.shard_map(
        per_device_fused,
        mesh=mesh,
        in_specs=(
            P(("outer", "inner"), None, None, None),
            P(("outer", "inner"), None, None, None),
            P(("outer", "inner"), None, None),
            P(("outer", "inner"), None, None),
            P(("outer", "inner"), None, None),
            P(("outer", "inner"), None, None),
            P(("outer", "inner"), None),
            P(("outer", "inner"), None, None),
        ),
        out_specs=(P(), P(("outer", "inner"), None, None), P(("outer", "inner"), None, None)),
        check_vma=False,
    )
```

```python
import functools
import math

import jax
import jax.numpy as jnp
from jax import lax
from jax.experimental import pallas as pl
from jax.experimental.pallas import tpu as pltpu
from jax.sharding import PartitionSpec as P

step_size = 0.0625


def select_blocks(resid, grad, ranks_flat, counts, owners, region, width):
    blocks = resid.shape[0]
    accum = (resid + grad.reshape(blocks, width)).reshape(owners, region, width)
    ranks = ranks_flat.reshape(owners, region)
    chosen = (ranks < counts[:, None])[..., None]
    new_resid = jnp.where(chosen, jnp.float32(0.0), accum).reshape(blocks, width)
    return (accum, ranks, chosen, new_resid)


def pack_slots(accum, ranks, counts, slots, region):
    order = lax.iota(jnp.int32, slots)
    picks = (ranks[:, None, :] == order[None, :, None]) & (
        order[None, :, None] < counts[:, None, None]
    )
    picks_f = picks.astype(jnp.float32)
    places = lax.iota(jnp.int32, region).astype(jnp.float32)
    packed = jnp.einsum("nkr,nrd->nkd", picks_f, accum, precision=lax.Precision.HIGHEST)
    where_at = jnp.einsum("nkr,r->nk", picks_f, places, precision=lax.Precision.HIGHEST)
    return (packed, where_at)


def unpack_slots(arrived, spots, region, width):
    places = lax.iota(jnp.int32, region).astype(jnp.float32)
    placed = (spots.reshape(-1)[:, None] == places[None, :]).astype(jnp.float32)
    return jnp.einsum(
        "mr,md->rd", placed, arrived.reshape(-1, width), precision=lax.Precision.HIGHEST
    )


def owner_section(pod_sum, oresid, ranks_out, count_out):
    owner_acc = pod_sum + oresid
    passed = (ranks_out < count_out)[:, None]
    outgoing = jnp.where(passed, owner_acc, jnp.float32(0.0))
    kept = jnp.where(passed, jnp.float32(0.0), owner_acc)
    return (outgoing, kept)


def per_device(acts, cotangent, residual, owner_residual, in_count, in_rank, out_count, out_rank):
    owners = lax.axis_size("inner")
    steps = acts.shape[1]
    tokens = acts.shape[2]
    rows = acts.shape[3]
    cols = cotangent.shape[3]
    blocks = residual.shape[1]
    width = residual.shape[2]
    region = blocks // owners
    slots = max(1, region // 2)
    scale = 1.0 / math.sqrt(tokens * owners)
    resid = residual[0]
    oresid = owner_residual[0]
    crosses = []
    packs = []
    spots_all = []
    for step in range(steps):
        grad = (
            jnp.einsum(
                "tr,tc->rc", acts[0, step], cotangent[0, step], preferred_element_type=jnp.float32
            )
            * scale
        )
        counts = in_count[0, step]
        accum, ranks, chosen, resid = select_blocks(
            resid, grad, in_rank[0, step], counts, owners, region, width
        )
        packed, where_at = pack_slots(accum, ranks, counts, slots, region)
        packs.append(packed)
        spots_all.append(where_at)
    arrived, spots = (
        lax.all_to_all(
            jnp.concatenate(packs, axis=1), "inner", split_axis=0, concat_axis=0, tiled=True
        ),
        lax.all_to_all(
            jnp.concatenate(spots_all, axis=1), "inner", split_axis=0, concat_axis=0, tiled=True
        ),
    )
    outgoings = []
    for step in range(steps):
        pod_sum = unpack_slots(
            arrived[:, step * slots : (step + 1) * slots],
            spots[:, step * slots : (step + 1) * slots],
            region,
            width,
        )
        outgoing, oresid = owner_section(pod_sum, oresid, out_rank[0, step], out_count[0, step])
        outgoings.append(outgoing)
    summed = lax.psum(jnp.stack(outgoings), "outer")
    for step in range(steps):
        crosses.append(summed[step])
    deltas = []
    for cross in crosses:
        delta = cross.astype(jnp.bfloat16)
        deltas.append(lax.all_gather(delta, "inner", axis=0, tiled=True))
    total = deltas[0].astype(jnp.float32)
    for later in deltas[1:]:
        total = total + later.astype(jnp.float32)
    applied = (-step_size * total).astype(jnp.bfloat16)
    return (applied.reshape(rows, cols), resid[None], oresid[None])


LANES = 128
F32 = jnp.float32
BF16 = jnp.bfloat16


def fused_kernel(
    dims,
    acts_hbm, cot_hbm, res_hbm, ores_hbm, cnt_hbm, rank_hbm, ocnt_hbm, orank_hbm,
    ag, resid_ref, nores_ref,
    ores_ref, cnt_ref, rank_ref, ocnt_ref, orank_ref,
    acts_v, cot_v, res_v, rk_ref, rp_ref, mt_ref, msend, mrecv,
    sent, psum, tsend, trecv, usend, urecv, osend, orecv, okeep,
    chosen_ref, sent_bytes, in_sem, s_sem, g_sem, mr_sem, sr_sem, tr_sem, zr_sem, fr_sem,
):
    n_in, n_out, steps, scale, region, width = dims
    rows, cols = acts_v.shape[2], cot_v.shape[2]
    cpr = cols // width
    rpr = region // cpr
    halves = region // LANES
    chunk = 2 * LANES
    rpc = chunk // rpr
    n_z = n_in // 2
    me = lax.axis_index("inner")
    pod = lax.axis_index("outer")
    core = lax.rem(me, 2)
    z = lax.div(me, 2)
    partner = me + 1 - 2 * core
    OVER_Z, KEPT, HAND, MASK, SHARE, TOTAL, GATHER_Z, GATHER_O = range(8)

    def flipped(at, m):
        v, bit = at, 1
        while bit <= m:
            if m & bit:
                v = v + bit - 2 * bit * lax.rem(lax.div(at, bit), 2)
            bit *= 2
        return v

    def flip(m):
        return flipped(z, m)

    def outer(d):
        return flipped(pod, d)

    def same_core(zz):
        return 2 * zz + core

    far_first = list(range(n_z - 1, 0, -1))
    far_pods = list(range(n_out - 1, 0, -1))

    def remote(src, dst, ssem, rsem, **device):
        return pltpu.make_async_remote_copy(
            src_ref=src, dst_ref=dst, send_sem=ssem, recv_sem=rsem,
            device_id=device, device_id_type=pl.DeviceIdType.MESH,
        )

    def send(phase, src, dst, rsem, **device):
        remote(src, dst, s_sem.at[0], rsem, **device).start()

    def arrived(ref, rsem):
        remote(ref, ref, s_sem.at[0], rsem, inner=partner).wait_recv()

    def left(phase, ref):
        remote(ref, ref, s_sem.at[0], g_sem.at[0], inner=partner).wait_send()

    barrier = pltpu.get_barrier_semaphore()
    for m in far_first:
        pl.semaphore_signal(barrier, inc=1, device_id={"inner": same_core(flip(m))}, device_id_type=pl.DeviceIdType.MESH)
    for d in far_pods:
        pl.semaphore_signal(barrier, inc=1, device_id={"outer": outer(d)}, device_id_type=pl.DeviceIdType.MESH)
        pl.semaphore_signal(barrier, inc=1, device_id={"outer": outer(d), "inner": partner}, device_id_type=pl.DeviceIdType.MESH)
    pl.semaphore_signal(barrier, inc=1, device_id={"inner": partner}, device_id_type=pl.DeviceIdType.MESH)

    small = [
        pltpu.make_async_copy(src, dst, in_sem.at[k])
        for k, (src, dst) in enumerate(
            ((rank_hbm, rank_ref), (cnt_hbm, cnt_ref), (orank_hbm, orank_ref), (ocnt_hbm, ocnt_ref), (ores_hbm, ores_ref))
        )
    ]
    for copy in small:
        copy.start()

    def fetch(s):
        pltpu.make_async_copy(acts_hbm.at[s], acts_v.at[s], in_sem.at[6 + s]).start()
        pltpu.make_async_copy(cot_hbm.at[s], cot_v.at[s], in_sem.at[6 + s]).start()

    fetch(0)
    res_load = pltpu.make_async_copy(res_hbm, res_v, in_sem.at[5])
    res_load.start()

    def loaded(s):
        both = acts_v.at[0:2]
        pltpu.make_async_copy(both, both, in_sem.at[6 + s]).wait()

    rk_ref[...] = jnp.zeros(rk_ref.shape, F32)
    msend[...] = jnp.zeros(msend.shape, F32)
    for copy in small:
        copy.wait()
    for s in range(1, steps):
        fetch(s)
    for s in range(steps):
        for j in range(n_in):
            row = rank_ref[s : s + 1, j * region : (j + 1) * region]
            rk_ref[s * n_in + j : s * n_in + j + 1, :] = jnp.where(row < cnt_ref[s : s + 1, j : j + 1], 1.0, 0.0)
    later = jnp.zeros((1, region), F32)
    for s in reversed(range(steps)):
        later = jnp.where(orank_ref[s : s + 1, :] < ocnt_ref[0:1, s : s + 1], 1.0, later)
        rk_ref[steps * n_in + s : steps * n_in + s + 1, :] = later
    old = lax.broadcasted_iota(jnp.int32, (region, region), 0)
    new = lax.broadcasted_iota(jnp.int32, (region, region), 1)
    shift = rpr.bit_length() - 1
    perm = jnp.where(old == (new & (rpr - 1)) * cpr + (new >> shift), 1.0, 0.0).astype(BF16)
    rp = jnp.dot(rk_ref[...].astype(BF16), perm, preferred_element_type=F32)
    rp_ref[...] = rp

    def eye(n):
        return jnp.where(
            lax.broadcasted_iota(jnp.int32, (n, LANES), 0) == lax.broadcasted_iota(jnp.int32, (n, LANES), 1), 1.0, 0.0
        ).astype(BF16)

    def turned(values):
        return lax.dot_general(
            values.astype(BF16), eye(values.shape[0]), (((0,), (0,)), ((), ())), preferred_element_type=F32
        ).astype(BF16)

    def spread(table, index, n):
        pick = jnp.where(lax.broadcasted_iota(jnp.int32, (LANES, n), 0) == index, 1.0, 0.0).astype(BF16)
        return jnp.dot(table, pick, preferred_element_type=F32)

    for s in range(steps):
        for h in range(halves):
            msend[s * halves + h : s * halves + h + 1, :] = rp_ref[
                steps * n_in + s : steps * n_in + s + 1, h * LANES : (h + 1) * LANES
            ]
    mt_ref[...] = turned(rp)
    for r in range(steps * n_in):
        chosen_ref[r] = spread(mt_ref[...], r, width)

    def greet():
        pl.semaphore_wait(barrier, n_z - 1 + n_out + n_out - 1)
        for m in far_first:
            send(MASK, msend, mrecv.at[z], mr_sem.at[m - 1], inner=same_core(flip(m)))

    def share(s, zz):
        send(SHARE, sent.at[s, 2 * zz + 1 - core], psum.at[s, zz], sr_sem.at[s], inner=partner)

    met = False
    waiting = []
    for s in range(steps):
        loaded(s)
        if s == 0:
            res_load.wait()
        for q in range(rows // chunk):
            g = lax.dot_general(
                acts_v[s, :, q * chunk : (q + 1) * chunk], cot_v[s], (((0,), (0,)), ((), ())),
                preferred_element_type=F32,
            ) * scale
            for half in range(rpc):
                j = q * rpc + half
                for c in range(cpr):
                    where_at = pl.ds(region * j + c, rpr, stride=cpr)
                    acc = res_v[where_at, :] + g[half * rpr : (half + 1) * rpr, c * width : (c + 1) * width]
                    take = chosen_ref[s * n_in + j, c * rpr : (c + 1) * rpr] > 0.5
                    (resid_ref if s == steps - 1 else res_v)[where_at, :] = jnp.where(take, 0.0, acc)
                    sent[s, j, c * rpr : (c + 1) * rpr] = jnp.where(take, acc, 0.0).astype(BF16)
            waiting += [(s, zz) for zz in range(q * rpc // 2, (q + 1) * rpc // 2)]
            if s == 0 and q == rows // chunk - 1:
                greet()
                met = True
            if met:
                for pair in waiting:
                    share(*pair)
                waiting = []

    for s in range(steps):
        arrived(psum.at[s], sr_sem.at[s])

    def passed(m, s):
        if m == 0:
            return spread(mt_ref[...], steps * n_in + s, width) > 0.5
        rows_of = mrecv[flip(m)].astype(BF16)
        parts = []
        for h in range(halves):
            pick = jnp.where(lax.broadcasted_iota(jnp.int32, (16, width), 0) == s * halves + h, 1.0, 0.0).astype(BF16)
            parts.append(lax.dot_general(rows_of, pick, (((0,), (0,)), ((), ())), preferred_element_type=F32))
        return jnp.concatenate(parts, axis=0) > 0.5

    def chip_sum(m, s):
        part = sent[s, same_core(flip(m))].astype(F32) + psum[s, flip(m)].astype(F32)
        if m == 0 and s == 0:
            part = part + jnp.concatenate([ores_ref[pl.ds(c, rpr, stride=cpr), :] for c in range(cpr)], axis=0)
        return part

    def send_total(m):
        zz = flip(m)
        t = jnp.zeros((region, width), F32)
        for s in range(steps):
            t = t + jnp.where(passed(m, s), chip_sum(m, s), 0.0)
        for q in range(n_out):
            tsend[zz, q] = t[q * rpr : (q + 1) * rpr].astype(BF16)
        for d in far_pods:
            send(TOTAL, tsend.at[zz, outer(d)], trecv.at[zz, pod], tr_sem.at[m], outer=outer(d))

    def keep(m):
        o = jnp.zeros((region, width), F32)
        for s in range(steps):
            o = o + jnp.where(passed(m, s), 0.0, chip_sum(m, s))
        return o

    def send_kept(m):
        osend[flip(m)] = keep(m).astype(BF16)
        send(KEPT, osend.at[flip(m)], orecv.at[z], g_sem.at[KEPT], inner=same_core(flip(m)))

    send_total(0)
    for m in reversed(far_first):
        arrived(mrecv.at[flip(m)], mr_sem.at[m - 1])
        send_total(m)
    late = n_z // 2
    for m in far_first:
        if m != late:
            send_kept(m)
    okeep[...] = keep(0)

    for m in far_first[::-1] + [0]:
        zz = flip(m)
        arrived(trecv.at[zz, 0 : n_out - 1], tr_sem.at[m])
        total = tsend[zz, pod].astype(F32)
        for d in far_pods:
            total = total + trecv[zz, outer(d)].astype(F32)
        if m:
            usend[zz] = total.astype(BF16)
            send(OVER_Z, usend.at[zz], urecv.at[z], g_sem.at[OVER_Z], inner=same_core(zz))
    arrived(urecv.at[0 : n_z - 1], g_sem.at[OVER_Z])
    for m in far_first:
        total = total + urecv[flip(m)].astype(F32)
    own = ag.at[pod, z, core]
    own[...] = (-step_size * total).astype(BF16)

    def forward(m):
        zz = flip(m)
        piece = ag.at[pod, zz, core]
        for d in far_pods:
            send(GATHER_O, piece, piece, fr_sem.at[m], outer=outer(d))

        if m == n_z - 1:
            for d in far_pods:
                send(GATHER_O, piece, piece, g_sem.at[HAND], outer=outer(d), inner=partner)

    def hand_over(q, m):
        piece = ag.at[q, flip(m), core]
        send(HAND, piece, piece, g_sem.at[HAND], inner=partner)

    for m in far_first:
        send(GATHER_Z, own, own, zr_sem.at[m - 1], inner=same_core(flip(m)))
    forward(0)
    hand_over(pod, 0)
    send_kept(late)

    for m in reversed(far_first):
        arrived(ag.at[pod, flip(m), core], zr_sem.at[m - 1])
        forward(m)
        hand_over(pod, m)
    for m in range(n_z):
        arrived(ag.at[0 : n_out - 1, flip(m), core], fr_sem.at[m])
        for d in far_pods:
            if m < n_z - 1:
                hand_over(outer(d), m)
    arrived(orecv.at[0 : n_z - 1], g_sem.at[KEPT])
    kept = okeep[...]
    for m in far_first:
        kept = kept + orecv[flip(m)].astype(F32)
    for c in range(cpr):
        nores_ref[pl.ds(c, rpr, stride=cpr), :] = kept[c * rpr : (c + 1) * rpr]

    arrived(ag.at[:, :, 1 - core], g_sem.at[HAND])
    left(0, sent_bytes)


def hand_out(pieces, *arrays):
    n = len(arrays)
    pods, rows, width = pieces.shape

    def kernel(*refs):
        src, dst, sems = refs[: n + 1], refs[n + 1 : 2 * n + 2], refs[2 * n + 2]
        copies = [pltpu.make_async_copy(src[k], dst[k], sems.at[k]) for k in range(1, n + 1)]
        copies += [
            pltpu.make_async_copy(src[0].at[q], dst[0].at[:, q * width : (q + 1) * width], sems.at[n + 1 + q])
            for q in range(pods)
        ]
        for copy in copies:
            copy.start()
        for copy in copies:
            copy.wait()

    return pl.pallas_call(
        kernel,
        out_shape=(jax.ShapeDtypeStruct((rows, pods * width), pieces.dtype),)
        + tuple(jax.ShapeDtypeStruct(a.shape, a.dtype) for a in arrays),
        in_specs=[pl.BlockSpec(memory_space=pltpu.VMEM)] * (n + 1),
        out_specs=tuple([pl.BlockSpec(memory_space=pltpu.HBM)] * (n + 1)),
        scratch_shapes=[pltpu.SemaphoreType.DMA((n + 1 + pods,))],
        compiler_params=pltpu.CompilerParams(vmem_limit_bytes=4 << 20),
    )(pieces, *arrays)


def fits(owners, pods, steps, rows, cols, blocks, width, region):
    if width != LANES or region % LANES or region > 256 or cols % width or owners % 4:
        return False
    cpr = cols // width
    rpr = region // cpr
    n_z = owners // 2
    return (
        cpr == pods and steps >= 2 and rows == cols and cpr * rpr == region and rpr % 16 == 0 and 2 * rpr == LANES
        and rows % (2 * LANES) == 0 and n_z & (n_z - 1) == 0 and pods & (pods - 1) == 0
        and rpr * owners == rows and steps * (owners + 1) <= LANES and steps * (region // LANES) <= 8
    )


def per_device_fused(acts, cotangent, residual, owner_residual, in_count, in_rank, out_count, out_rank):
    n_in = lax.axis_size("inner")
    n_out = lax.axis_size("outer")
    steps, tokens, rows = acts.shape[1:]
    cols = cotangent.shape[3]
    blocks, width = residual.shape[1:]
    region = blocks // n_in
    if not fits(n_in, n_out, steps, rows, cols, blocks, width, region):
        return per_device(acts, cotangent, residual, owner_residual, in_count, in_rank, out_count, out_rank)
    scale = 1.0 / math.sqrt(tokens * n_in)
    rpr = region // n_out
    n_z = n_in // 2
    n_rk = -(-steps * (n_in + 1) // 16) * 16
    piece = rpr // 2
    n_sent = (n_z - 1) * (16 + 2 * piece + region // 2) + steps * n_z * region // 2
    n_sent += 2 * n_z * (n_out - 1) * piece + n_z * n_out * piece
    vmem = pl.BlockSpec(memory_space=pltpu.VMEM)
    anywhere = pl.BlockSpec(memory_space=pltpu.HBM)
    dma = pltpu.SemaphoreType.DMA
    pieces, resid, oresid = pl.pallas_call(
        functools.partial(fused_kernel, (n_in, n_out, steps, scale, region, width)),
        out_shape=(
            jax.ShapeDtypeStruct((n_out, n_z, 2, rpr, width), BF16),
            jax.ShapeDtypeStruct((blocks, width), F32),
            jax.ShapeDtypeStruct((region, width), F32),
        ),
        in_specs=[anywhere] * 8,
        out_specs=(vmem, vmem, vmem),
        scratch_shapes=[
            pltpu.VMEM((region, width), F32),
            pltpu.VMEM((steps, n_in), jnp.int32),
            pltpu.VMEM((steps, blocks), jnp.int32),
            pltpu.VMEM((1, steps), jnp.int32),
            pltpu.VMEM((steps, region), jnp.int32),
            pltpu.VMEM((steps, tokens, rows), BF16),
            pltpu.VMEM((steps, tokens, cols), BF16),
            pltpu.VMEM((blocks, width), F32),
            pltpu.VMEM((n_rk, region), F32),
            pltpu.VMEM((n_rk, region), F32),
            pltpu.VMEM((region, LANES), BF16),
            pltpu.VMEM((16, LANES), F32),
            pltpu.VMEM((n_z, 16, LANES), F32),
            pltpu.VMEM((steps, n_in, region, width), BF16),
            pltpu.VMEM((steps, n_z, region, width), BF16),
            pltpu.VMEM((n_z, n_out, rpr, width), BF16),
            pltpu.VMEM((n_z, n_out, rpr, width), BF16),
            pltpu.VMEM((n_z, rpr, width), BF16),
            pltpu.VMEM((n_z, rpr, width), BF16),
            pltpu.VMEM((n_z, region, width), BF16),
            pltpu.VMEM((n_z, region, width), BF16),
            pltpu.VMEM((region, width), F32),
            pltpu.VMEM((steps * n_in, region, width), F32),
            pltpu.VMEM((n_sent, LANES), F32),
            dma((6 + steps,)),
            dma((1,)),
            dma((3,)),
            dma((n_z - 1,)),
            dma((steps,)),
            dma((n_z,)),
            dma((n_z - 1,)),
            dma((n_z,)),
        ],
        compiler_params=pltpu.CompilerParams(collective_id=0, has_side_effects=True, vmem_limit_bytes=48 << 20),
    )(*(
        pltpu.with_memory_space_constraint(a, pltpu.HBM)
        for a in (
            acts[0], cotangent[0], residual[0], owner_residual[0], in_count[0], in_rank[0], out_count, out_rank[0]
        )
    ))
    applied, resid, oresid = hand_out(pieces.reshape(n_out, rows, width), resid, oresid)
    return applied, resid[None], oresid[None]


def solution(mesh):
    return jax.shard_map(
        per_device_fused,
        mesh=mesh,
        in_specs=(
            P(("outer", "inner"), None, None, None),
            P(("outer", "inner"), None, None, None),
            P(("outer", "inner"), None, None),
            P(("outer", "inner"), None, None),
            P(("outer", "inner"), None, None),
            P(("outer", "inner"), None, None),
            P(("outer", "inner"), None),
            P(("outer", "inner"), None, None),
        ),
        out_specs=(P(), P(("outer", "inner"), None, None), P(("outer", "inner"), None, None)),
        check_vma=False,
    )
```

```python
import functools
import math

import jax
import jax.numpy as jnp
from jax import lax
from jax.experimental import pallas as pl
from jax.experimental.pallas import tpu as pltpu
from jax.sharding import PartitionSpec as P

step_size = 0.0625


def select_blocks(resid, grad, ranks_flat, counts, owners, region, width):
    blocks = resid.shape[0]
    accum = (resid + grad.reshape(blocks, width)).reshape(owners, region, width)
    ranks = ranks_flat.reshape(owners, region)
    chosen = (ranks < counts[:, None])[..., None]
    new_resid = jnp.where(chosen, jnp.float32(0.0), accum).reshape(blocks, width)
    return (accum, ranks, chosen, new_resid)


def pack_slots(accum, ranks, counts, slots, region):
    order = lax.iota(jnp.int32, slots)
    picks = (ranks[:, None, :] == order[None, :, None]) & (
        order[None, :, None] < counts[:, None, None]
    )
    picks_f = picks.astype(jnp.float32)
    places = lax.iota(jnp.int32, region).astype(jnp.float32)
    packed = jnp.einsum("nkr,nrd->nkd", picks_f, accum, precision=lax.Precision.HIGHEST)
    where_at = jnp.einsum("nkr,r->nk", picks_f, places, precision=lax.Precision.HIGHEST)
    return (packed, where_at)


def unpack_slots(arrived, spots, region, width):
    places = lax.iota(jnp.int32, region).astype(jnp.float32)
    placed = (spots.reshape(-1)[:, None] == places[None, :]).astype(jnp.float32)
    return jnp.einsum(
        "mr,md->rd", placed, arrived.reshape(-1, width), precision=lax.Precision.HIGHEST
    )


def owner_section(pod_sum, oresid, ranks_out, count_out):
    owner_acc = pod_sum + oresid
    passed = (ranks_out < count_out)[:, None]
    outgoing = jnp.where(passed, owner_acc, jnp.float32(0.0))
    kept = jnp.where(passed, jnp.float32(0.0), owner_acc)
    return (outgoing, kept)


def per_device(acts, cotangent, residual, owner_residual, in_count, in_rank, out_count, out_rank):
    owners = lax.axis_size("inner")
    steps = acts.shape[1]
    tokens = acts.shape[2]
    rows = acts.shape[3]
    cols = cotangent.shape[3]
    blocks = residual.shape[1]
    width = residual.shape[2]
    region = blocks // owners
    slots = max(1, region // 2)
    scale = 1.0 / math.sqrt(tokens * owners)
    resid = residual[0]
    oresid = owner_residual[0]
    crosses = []
    packs = []
    spots_all = []
    for step in range(steps):
        grad = (
            jnp.einsum(
                "tr,tc->rc", acts[0, step], cotangent[0, step], preferred_element_type=jnp.float32
            )
            * scale
        )
        counts = in_count[0, step]
        accum, ranks, chosen, resid = select_blocks(
            resid, grad, in_rank[0, step], counts, owners, region, width
        )
        packed, where_at = pack_slots(accum, ranks, counts, slots, region)
        packs.append(packed)
        spots_all.append(where_at)
    arrived, spots = (
        lax.all_to_all(
            jnp.concatenate(packs, axis=1), "inner", split_axis=0, concat_axis=0, tiled=True
        ),
        lax.all_to_all(
            jnp.concatenate(spots_all, axis=1), "inner", split_axis=0, concat_axis=0, tiled=True
        ),
    )
    outgoings = []
    for step in range(steps):
        pod_sum = unpack_slots(
            arrived[:, step * slots : (step + 1) * slots],
            spots[:, step * slots : (step + 1) * slots],
            region,
            width,
        )
        outgoing, oresid = owner_section(pod_sum, oresid, out_rank[0, step], out_count[0, step])
        outgoings.append(outgoing)
    summed = lax.psum(jnp.stack(outgoings), "outer")
    for step in range(steps):
        crosses.append(summed[step])
    deltas = []
    for cross in crosses:
        delta = cross.astype(jnp.bfloat16)
        deltas.append(lax.all_gather(delta, "inner", axis=0, tiled=True))
    total = deltas[0].astype(jnp.float32)
    for later in deltas[1:]:
        total = total + later.astype(jnp.float32)
    applied = (-step_size * total).astype(jnp.bfloat16)
    return (applied.reshape(rows, cols), resid[None], oresid[None])


LANES = 128
F32 = jnp.float32
BF16 = jnp.bfloat16


def fused_kernel(
    dims,
    acts_hbm, cot_hbm, res_hbm, ores_hbm, cnt_hbm, rank_hbm, ocnt_hbm, orank_hbm,
    ag, resid_ref, nores_ref,
    ores_ref, cnt_ref, rank_ref, ocnt_ref, orank_ref,
    acts_v, cot_v, res_v, rk_ref, rp_ref, mt_ref, msend, mrecv,
    sent, psum, tsend, trecv, usend, urecv, osend, orecv, okeep,
    chosen_ref, sent_bytes, in_sem, s_sem, g_sem, mr_sem, sr_sem, tr_sem, zr_sem, fr_sem,
):
    n_in, n_out, steps, scale, region, width = dims
    rows, cols = acts_v.shape[2], cot_v.shape[2]
    cpr = cols // width
    rpr = region // cpr
    halves = region // LANES
    chunk = 2 * LANES
    rpc = chunk // rpr
    n_z = n_in // 2
    me = lax.axis_index("inner")
    pod = lax.axis_index("outer")
    core = lax.rem(me, 2)
    z = lax.div(me, 2)
    partner = me + 1 - 2 * core
    OVER_Z, KEPT, HAND, MASK, SHARE, TOTAL, GATHER_Z, GATHER_O = range(8)

    def flipped(at, m):
        v, bit = at, 1
        while bit <= m:
            if m & bit:
                v = v + bit - 2 * bit * lax.rem(lax.div(at, bit), 2)
            bit *= 2
        return v

    def flip(m):
        return flipped(z, m)

    def outer(d):
        return flipped(pod, d)

    def same_core(zz):
        return 2 * zz + core

    far_first = list(range(n_z - 1, 0, -1))
    far_pods = list(range(n_out - 1, 0, -1))

    def remote(src, dst, ssem, rsem, **device):
        return pltpu.make_async_remote_copy(
            src_ref=src, dst_ref=dst, send_sem=ssem, recv_sem=rsem,
            device_id=device, device_id_type=pl.DeviceIdType.MESH,
        )

    def send(phase, src, dst, rsem, **device):
        remote(src, dst, s_sem.at[0], rsem, **device).start()

    def arrived(ref, rsem):
        remote(ref, ref, s_sem.at[0], rsem, inner=partner).wait_recv()

    def left(phase, ref):
        remote(ref, ref, s_sem.at[0], g_sem.at[0], inner=partner).wait_send()

    barrier = pltpu.get_barrier_semaphore()
    for m in far_first:
        pl.semaphore_signal(barrier, inc=1, device_id={"inner": same_core(flip(m))}, device_id_type=pl.DeviceIdType.MESH)
    for d in far_pods:
        pl.semaphore_signal(barrier, inc=1, device_id={"outer": outer(d)}, device_id_type=pl.DeviceIdType.MESH)
        pl.semaphore_signal(barrier, inc=1, device_id={"outer": outer(d), "inner": partner}, device_id_type=pl.DeviceIdType.MESH)
    pl.semaphore_signal(barrier, inc=1, device_id={"inner": partner}, device_id_type=pl.DeviceIdType.MESH)

    small = [
        pltpu.make_async_copy(src, dst, in_sem.at[k])
        for k, (src, dst) in enumerate(
            ((rank_hbm, rank_ref), (cnt_hbm, cnt_ref), (orank_hbm, orank_ref), (ocnt_hbm, ocnt_ref), (ores_hbm, ores_ref))
        )
    ]
    for copy in small:
        copy.start()

    def fetch(s):
        pltpu.make_async_copy(acts_hbm.at[s], acts_v.at[s], in_sem.at[6 + s]).start()
        pltpu.make_async_copy(cot_hbm.at[s], cot_v.at[s], in_sem.at[6 + s]).start()

    fetch(0)
    res_load = pltpu.make_async_copy(res_hbm, res_v, in_sem.at[5])
    res_load.start()

    def loaded(s):
        both = acts_v.at[0:2]
        pltpu.make_async_copy(both, both, in_sem.at[6 + s]).wait()

    rk_ref[...] = jnp.zeros(rk_ref.shape, F32)
    msend[...] = jnp.zeros(msend.shape, F32)
    for copy in small:
        copy.wait()
    for s in range(1, steps):
        fetch(s)
    for s in range(steps):
        for j in range(n_in):
            row = rank_ref[s : s + 1, j * region : (j + 1) * region]
            rk_ref[s * n_in + j : s * n_in + j + 1, :] = jnp.where(row < cnt_ref[s : s + 1, j : j + 1], 1.0, 0.0)
    later = jnp.zeros((1, region), F32)
    for s in reversed(range(steps)):
        later = jnp.where(orank_ref[s : s + 1, :] < ocnt_ref[0:1, s : s + 1], 1.0, later)
        rk_ref[steps * n_in + s : steps * n_in + s + 1, :] = later
    old = lax.broadcasted_iota(jnp.int32, (region, region), 0)
    new = lax.broadcasted_iota(jnp.int32, (region, region), 1)
    shift = rpr.bit_length() - 1
    perm = jnp.where(old == (new & (rpr - 1)) * cpr + (new >> shift), 1.0, 0.0).astype(BF16)
    rp = jnp.dot(rk_ref[...].astype(BF16), perm, preferred_element_type=F32)
    rp_ref[...] = rp

    def eye(n):
        return jnp.where(
            lax.broadcasted_iota(jnp.int32, (n, LANES), 0) == lax.broadcasted_iota(jnp.int32, (n, LANES), 1), 1.0, 0.0
        ).astype(BF16)

    def turned(values):
        return lax.dot_general(
            values.astype(BF16), eye(values.shape[0]), (((0,), (0,)), ((), ())), preferred_element_type=F32
        ).astype(BF16)

    def spread(table, index, n):
        pick = jnp.where(lax.broadcasted_iota(jnp.int32, (LANES, n), 0) == index, 1.0, 0.0).astype(BF16)
        return jnp.dot(table, pick, preferred_element_type=F32)

    for s in range(steps):
        for h in range(halves):
            msend[s * halves + h : s * halves + h + 1, :] = rp_ref[
                steps * n_in + s : steps * n_in + s + 1, h * LANES : (h + 1) * LANES
            ]
    mt_ref[...] = turned(rp)
    for r in range(steps * n_in):
        chosen_ref[r] = spread(mt_ref[...], r, width)

    def greet():
        pl.semaphore_wait(barrier, n_z - 1 + n_out + n_out - 1)
        for m in far_first:
            send(MASK, msend, mrecv.at[z], mr_sem.at[m - 1], inner=same_core(flip(m)))

    def share(s, zz):
        send(SHARE, sent.at[s, 2 * zz + 1 - core], psum.at[s, zz], sr_sem.at[s], inner=partner)

    met = False
    waiting = []
    for s in range(steps):
        loaded(s)
        if s == 0:
            res_load.wait()
        for q in range(rows // chunk):
            g = lax.dot_general(
                acts_v[s, :, q * chunk : (q + 1) * chunk], cot_v[s], (((0,), (0,)), ((), ())),
                preferred_element_type=F32,
            ) * scale
            for half in range(rpc):
                j = q * rpc + half
                for c in range(cpr):
                    where_at = pl.ds(region * j + c, rpr, stride=cpr)
                    acc = res_v[where_at, :] + g[half * rpr : (half + 1) * rpr, c * width : (c + 1) * width]
                    take = chosen_ref[s * n_in + j, c * rpr : (c + 1) * rpr] > 0.5
                    (resid_ref if s == steps - 1 else res_v)[where_at, :] = jnp.where(take, 0.0, acc)
                    sent[s, j, c * rpr : (c + 1) * rpr] = jnp.where(take, acc, 0.0).astype(BF16)
            waiting += [(s, zz) for zz in range(q * rpc // 2, (q + 1) * rpc // 2)]
            if s == 0 and q == rows // chunk - 1:
                greet()
                met = True
            if met:
                for pair in waiting:
                    share(*pair)
                waiting = []

    for s in range(steps):
        arrived(psum.at[s], sr_sem.at[s])

    def passed(m, s):
        if m == 0:
            return spread(mt_ref[...], steps * n_in + s, width) > 0.5
        rows_of = mrecv[flip(m)].astype(BF16)
        parts = []
        for h in range(halves):
            pick = jnp.where(lax.broadcasted_iota(jnp.int32, (16, width), 0) == s * halves + h, 1.0, 0.0).astype(BF16)
            parts.append(lax.dot_general(rows_of, pick, (((0,), (0,)), ((), ())), preferred_element_type=F32))
        return jnp.concatenate(parts, axis=0) > 0.5

    def chip_sum(m, s):
        part = sent[s, same_core(flip(m))].astype(F32) + psum[s, flip(m)].astype(F32)
        if m == 0 and s == 0:
            part = part + jnp.concatenate([ores_ref[pl.ds(c, rpr, stride=cpr), :] for c in range(cpr)], axis=0)
        return part

    def send_total(m):
        zz = flip(m)
        t = jnp.zeros((region, width), F32)
        for s in range(steps):
            t = t + jnp.where(passed(m, s), chip_sum(m, s), 0.0)
        for q in range(n_out):
            tsend[zz, q] = t[q * rpr : (q + 1) * rpr].astype(BF16)
        for d in far_pods:
            send(TOTAL, tsend.at[zz, outer(d)], trecv.at[zz, pod], tr_sem.at[m], outer=outer(d))

    def keep(m):
        o = jnp.zeros((region, width), F32)
        for s in range(steps):
            o = o + jnp.where(passed(m, s), 0.0, chip_sum(m, s))
        return o

    def send_kept(m):
        osend[flip(m)] = keep(m).astype(BF16)
        send(KEPT, osend.at[flip(m)], orecv.at[z], g_sem.at[KEPT], inner=same_core(flip(m)))

    late = n_z // 2
    turns = [late] + [m for m in far_first if m != late]
    for m in turns:
        arrived(mrecv.at[flip(m)], mr_sem.at[m - 1])
        send_total(m)
    send_total(0)
    for m in far_first:
        if m != late:
            send_kept(m)
    okeep[...] = keep(0)

    for m in turns + [0]:
        zz = flip(m)
        arrived(trecv.at[zz, 0 : n_out - 1], tr_sem.at[m])
        total = tsend[zz, pod].astype(F32)
        for d in far_pods:
            total = total + trecv[zz, outer(d)].astype(F32)
        if m:
            usend[zz] = total.astype(BF16)
            send(OVER_Z, usend.at[zz], urecv.at[z], g_sem.at[OVER_Z], inner=same_core(zz))
    arrived(urecv.at[0 : n_z - 1], g_sem.at[OVER_Z])
    for m in far_first:
        total = total + urecv[flip(m)].astype(F32)
    own = ag.at[pod, z, core]
    own[...] = (-step_size * total).astype(BF16)

    def forward(m):
        zz = flip(m)
        piece = ag.at[pod, zz, core]
        for d in far_pods:
            send(GATHER_O, piece, piece, fr_sem.at[m], outer=outer(d))

        if m == n_z - 1:
            for d in far_pods:
                send(GATHER_O, piece, piece, g_sem.at[HAND], outer=outer(d), inner=partner)

    def hand_over(q, m):
        piece = ag.at[q, flip(m), core]
        send(HAND, piece, piece, g_sem.at[HAND], inner=partner)

    for m in far_first:
        send(GATHER_Z, own, own, zr_sem.at[m - 1], inner=same_core(flip(m)))
    forward(0)
    hand_over(pod, 0)
    send_kept(late)

    for m in reversed(far_first):
        arrived(ag.at[pod, flip(m), core], zr_sem.at[m - 1])
        forward(m)
        hand_over(pod, m)
    for m in range(n_z):
        arrived(ag.at[0 : n_out - 1, flip(m), core], fr_sem.at[m])
        for d in far_pods:
            if m < n_z - 1:
                hand_over(outer(d), m)
    arrived(orecv.at[0 : n_z - 1], g_sem.at[KEPT])
    kept = okeep[...]
    for m in far_first:
        kept = kept + orecv[flip(m)].astype(F32)
    for c in range(cpr):
        nores_ref[pl.ds(c, rpr, stride=cpr), :] = kept[c * rpr : (c + 1) * rpr]

    arrived(ag.at[:, :, 1 - core], g_sem.at[HAND])
    left(0, sent_bytes)


def hand_out(pieces, *arrays):
    n = len(arrays)
    pods, rows, width = pieces.shape

    def kernel(*refs):
        src, dst, sems = refs[: n + 1], refs[n + 1 : 2 * n + 2], refs[2 * n + 2]
        copies = [pltpu.make_async_copy(src[k], dst[k], sems.at[k]) for k in range(1, n + 1)]
        copies += [
            pltpu.make_async_copy(src[0].at[q], dst[0].at[:, q * width : (q + 1) * width], sems.at[n + 1 + q])
            for q in range(pods)
        ]
        for copy in copies:
            copy.start()
        for copy in copies:
            copy.wait()

    return pl.pallas_call(
        kernel,
        out_shape=(jax.ShapeDtypeStruct((rows, pods * width), pieces.dtype),)
        + tuple(jax.ShapeDtypeStruct(a.shape, a.dtype) for a in arrays),
        in_specs=[pl.BlockSpec(memory_space=pltpu.VMEM)] * (n + 1),
        out_specs=tuple([pl.BlockSpec(memory_space=pltpu.HBM)] * (n + 1)),
        scratch_shapes=[pltpu.SemaphoreType.DMA((n + 1 + pods,))],
        compiler_params=pltpu.CompilerParams(vmem_limit_bytes=4 << 20),
    )(pieces, *arrays)


def fits(owners, pods, steps, rows, cols, blocks, width, region):
    if width != LANES or region % LANES or region > 256 or cols % width or owners % 4:
        return False
    cpr = cols // width
    rpr = region // cpr
    n_z = owners // 2
    return (
        cpr == pods and steps >= 2 and rows == cols and cpr * rpr == region and rpr % 16 == 0 and 2 * rpr == LANES
        and rows % (2 * LANES) == 0 and n_z & (n_z - 1) == 0 and pods & (pods - 1) == 0
        and rpr * owners == rows and steps * (owners + 1) <= LANES and steps * (region // LANES) <= 8
    )


def per_device_fused(acts, cotangent, residual, owner_residual, in_count, in_rank, out_count, out_rank):
    n_in = lax.axis_size("inner")
    n_out = lax.axis_size("outer")
    steps, tokens, rows = acts.shape[1:]
    cols = cotangent.shape[3]
    blocks, width = residual.shape[1:]
    region = blocks // n_in
    if not fits(n_in, n_out, steps, rows, cols, blocks, width, region):
        return per_device(acts, cotangent, residual, owner_residual, in_count, in_rank, out_count, out_rank)
    scale = 1.0 / math.sqrt(tokens * n_in)
    rpr = region // n_out
    n_z = n_in // 2
    n_rk = -(-steps * (n_in + 1) // 16) * 16
    piece = rpr // 2
    n_sent = (n_z - 1) * (16 + 2 * piece + region // 2) + steps * n_z * region // 2
    n_sent += 2 * n_z * (n_out - 1) * piece + n_z * n_out * piece
    vmem = pl.BlockSpec(memory_space=pltpu.VMEM)
    anywhere = pl.BlockSpec(memory_space=pltpu.HBM)
    dma = pltpu.SemaphoreType.DMA
    pieces, resid, oresid = pl.pallas_call(
        functools.partial(fused_kernel, (n_in, n_out, steps, scale, region, width)),
        out_shape=(
            jax.ShapeDtypeStruct((n_out, n_z, 2, rpr, width), BF16),
            jax.ShapeDtypeStruct((blocks, width), F32),
            jax.ShapeDtypeStruct((region, width), F32),
        ),
        in_specs=[anywhere] * 8,
        out_specs=(vmem, vmem, vmem),
        scratch_shapes=[
            pltpu.VMEM((region, width), F32),
            pltpu.VMEM((steps, n_in), jnp.int32),
            pltpu.VMEM((steps, blocks), jnp.int32),
            pltpu.VMEM((1, steps), jnp.int32),
            pltpu.VMEM((steps, region), jnp.int32),
            pltpu.VMEM((steps, tokens, rows), BF16),
            pltpu.VMEM((steps, tokens, cols), BF16),
            pltpu.VMEM((blocks, width), F32),
            pltpu.VMEM((n_rk, region), F32),
            pltpu.VMEM((n_rk, region), F32),
            pltpu.VMEM((region, LANES), BF16),
            pltpu.VMEM((16, LANES), F32),
            pltpu.VMEM((n_z, 16, LANES), F32),
            pltpu.VMEM((steps, n_in, region, width), BF16),
            pltpu.VMEM((steps, n_z, region, width), BF16),
            pltpu.VMEM((n_z, n_out, rpr, width), BF16),
            pltpu.VMEM((n_z, n_out, rpr, width), BF16),
            pltpu.VMEM((n_z, rpr, width), BF16),
            pltpu.VMEM((n_z, rpr, width), BF16),
            pltpu.VMEM((n_z, region, width), BF16),
            pltpu.VMEM((n_z, region, width), BF16),
            pltpu.VMEM((region, width), F32),
            pltpu.VMEM((steps * n_in, region, width), F32),
            pltpu.VMEM((n_sent, LANES), F32),
            dma((6 + steps,)),
            dma((1,)),
            dma((3,)),
            dma((n_z - 1,)),
            dma((steps,)),
            dma((n_z,)),
            dma((n_z - 1,)),
            dma((n_z,)),
        ],
        compiler_params=pltpu.CompilerParams(collective_id=0, has_side_effects=True, vmem_limit_bytes=48 << 20),
    )(*(
        pltpu.with_memory_space_constraint(a, pltpu.HBM)
        for a in (
            acts[0], cotangent[0], residual[0], owner_residual[0], in_count[0], in_rank[0], out_count, out_rank[0]
        )
    ))
    applied, resid, oresid = hand_out(pieces.reshape(n_out, rows, width), resid, oresid)
    return applied, resid[None], oresid[None]


def solution(mesh):
    return jax.shard_map(
        per_device_fused,
        mesh=mesh,
        in_specs=(
            P(("outer", "inner"), None, None, None),
            P(("outer", "inner"), None, None, None),
            P(("outer", "inner"), None, None),
            P(("outer", "inner"), None, None),
            P(("outer", "inner"), None, None),
            P(("outer", "inner"), None, None),
            P(("outer", "inner"), None),
            P(("outer", "inner"), None, None),
        ),
        out_specs=(P(), P(("outer", "inner"), None, None), P(("outer", "inner"), None, None)),
        check_vma=False,
    )
```
